32 devices in a mesh: texel: 8 (over y, x, core), light: 4 (over z).
Axes of the slice: x: 2, y: 2, z: 4, core: 2. Of those that a mesh axis runs over, the one named last changes fastest.
Arguments:
- tex_feat: bfloat16 [8192, 512], P('texel'), may hold values from -18 to 18
- light_feat: bfloat16 [6144, 512], P('light'), may hold values from -0.25 to 0.25
- sketch: bfloat16 [6144, 256], P('light'), may hold values from -0.078125 to 0.078125
- row_counts: int32 [8], replicated, may hold values from 1 to 1024, 4096 in all
Outputs:
- basis: float32 [8192, 256], P('texel')
- coeffs: float32 [256, 6144], P('texel', 'light')
The draws below stay inside these ranges and needn't reach their ends.
Inputs may be any that keep to these rules, and one draw needn't show every extreme that they name: row_counts sums to 8 * 512; some entry equals 1024.
All inputs are finite; a program needn't handle non-finite values.
Results may differ from the reference program's by a relative error of at most 0.0034.
Values sent between devices are 32-bit elements; how exact they have to be, the bound alone decides.
A program may use at most 64 MiB of HBM per device.

```python
import math
import jax
import jax.numpy as jnp
import numpy as np
from jax import lax

F = 512
K = 256
CAP = 1024
LIGHT_DEV = 1536
TEX_SLOTS = 8192
LIGHTS = 6144
N_TEXEL = 8
N_LIGHT = 4


def level_of(key, extent, cuts, low, largest):
    def one(axis_at, parts):
        heights = jax.random.uniform(jax.random.fold_in(jax.random.fold_in(key, 6), axis_at), (parts,), jnp.float32, low / len(cuts), largest / len(cuts))
        return jnp.repeat(jnp.exp(heights), extent[axis_at] // parts).reshape((-1,) + (1,) * (len(extent) - axis_at - 1))

    factor_of = one(*cuts[0])
    for cut in cuts[1:]:
        factor_of = factor_of * one(*cut)
    return factor_of


def split_up(count, total, reach, slope):
    loads = [(1 << 20) // math.isqrt(grade ** slope) + 1 for grade in range(2, count + 1)]
    surplus, counts = total - reach - (count - 1), [1] * (count - 1)
    while surplus > 0:
        free = [i for i in range(count - 1) if counts[i] < reach]
        mass, remaining = sum([loads[i] for i in free]), surplus
        for i in free:
            extra = min(reach - counts[i], max(1, remaining * loads[i] // mass), surplus)
            counts[i] = counts[i] + extra
            surplus = surplus - extra
    return np.array([reach] + counts)


def ragged_sizes(own_key, amount, total, bound, slope):
    if amount == 2:
        one = jax.random.randint(own_key, (), max(1, total - bound), min(bound, total - 1) + 1)
        return jnp.stack([one, total - one])
    tallies = jnp.asarray(split_up(amount, total, bound, slope), jnp.int32)
    twos = (amount - 1) // 2
    source_of, sink = tallies[1:1 + 2 * twos:2], tallies[2:2 + 2 * twos:2]
    margin = jnp.minimum(source_of - 1, bound - sink)
    passed = jax.random.randint(jax.random.fold_in(own_key, 1), (twos,), 0, 1 << 20) % (margin + 1)
    tallies = tallies.at[1:1 + 2 * twos:2].set(source_of - passed).at[2:2 + 2 * twos:2].set(sink + passed)
    return tallies[jax.random.permutation(jax.random.fold_in(own_key, 2), amount)]


def scatter_about(key, dims, scale, limit, split=(), kind=jnp.bfloat16):
    factor_of = level_of(key, dims, split, -0.22, 0.18) if split else 1.0
    entries = jax.random.normal(key, dims, jnp.float32) * scale * factor_of
    return jnp.minimum(jnp.maximum(entries, -limit), limit).astype(kind)


def setup_inputs(seed: int = 0) -> dict:
    arg_keys = jax.random.split(jax.random.key(seed), 5)
    return {
        "tex_feat": scatter_about(arg_keys[0], (TEX_SLOTS, F), 3.0, 18.0, ((0, 8),)),
        "light_feat": scatter_about(arg_keys[1], (LIGHTS, F), F ** -0.5, 0.25, ((0, 4),)),
        "sketch": scatter_about(arg_keys[2], (LIGHTS, K), LIGHTS ** -0.5, 0.078125, ((0, 4),)),
        "row_counts": ragged_sizes(arg_keys[3], N_TEXEL, N_TEXEL * CAP // 2, CAP, 2).astype(jnp.int32),
    }


def reference(tex_feat, light_feat, sketch, row_counts):
    slot_total = tex_feat.shape[0]
    positions = lax.iota(jnp.int32, slot_total)
    owners = (positions // CAP).astype(jnp.int32)
    row_valid = (positions % CAP < row_counts[owners]).astype(jnp.float32)
    valid_total = jnp.sum(row_counts).astype(jnp.float32)
    light_blocks = light_feat.reshape(N_LIGHT, LIGHT_DEV, F)
    sketch_blocks = sketch.reshape(N_LIGHT, LIGHT_DEV, K)

    def make_tiles(feats):
        logits = lax.dot_general(tex_feat.astype(jnp.float32), feats.astype(jnp.float32), (((1,), (1,)), ((), ())), preferred_element_type=jnp.float32)
        return jnp.sin(logits).astype(jnp.bfloat16)

    def accumulate(carry, pair):
        feats, block = pair
        return (carry + jnp.dot(make_tiles(feats).astype(jnp.float32), block.astype(jnp.float32), preferred_element_type=jnp.float32), None)
    sketched, _ = lax.scan(accumulate, jnp.zeros((slot_total, K), jnp.float32), (light_blocks, sketch_blocks))
    sketched = sketched * row_valid[:, None]
    gram_matrix = jnp.dot(sketched.T, sketched, precision=lax.Precision.HIGHEST) / valid_total
    factor = jnp.linalg.cholesky(gram_matrix)
    basis = jax.scipy.linalg.solve_triangular(factor, sketched.T, lower=True).T
    basis_half = basis.astype(jnp.bfloat16)

    def project(feats):
        return lax.dot_general(basis_half.astype(jnp.float32), make_tiles(feats).astype(jnp.float32), (((0,), (0,)), ((), ())), preferred_element_type=jnp.float32)
    coeff_blocks = lax.map(project, light_blocks)
    coeffs = jnp.transpose(coeff_blocks, (1, 0, 2)).reshape(K, N_LIGHT * LIGHT_DEV) / jnp.sqrt(valid_total)
    return (basis, coeffs)
```

```python
import functools

import jax
import jax.numpy as jnp
from jax import lax
from jax.experimental import pallas as pl
from jax.experimental.pallas import tpu as pltpu
from jax.sharding import PartitionSpec as P

HIGHEST = lax.Precision.HIGHEST
BLOCK = 64
INV_TWO_PI = 0.15915494309189535
TWO_PI_HIGH = 6.28125
TWO_PI_LOW = 0.001935307179586232
SINE = (
    0.9999999944783076,
    -0.16666664569596037,
    0.008333310280569169,
    -0.00019840151040396647,
    2.752937413742719e-06,
    -2.4676261406891767e-08,
    1.344908473337278e-10,
)


def bounded_sine(x):
    turns = jnp.round(x * INV_TWO_PI)
    r = (x - turns * TWO_PI_HIGH) - turns * TWO_PI_LOW
    s = r * r
    value = jnp.full_like(s, SINE[-1])
    for coefficient in SINE[-2::-1]:
        value = value * s + coefficient
    return value * r


def eliminate(block):
    rows = [block[8 * t : 8 * t + 8, :] for t in range(8)]
    below = lax.broadcasted_iota(jnp.int32, (8, 128), 0)
    for p in range(8):
        columns = {
            (t, k): jnp.broadcast_to(rows[t][:, 8 * p + k : 8 * p + k + 1], (8, 128))
            for t in range(p, 8)
            for k in range(8)
        }
        for k in range(8):
            inverse = 1.0 / jnp.broadcast_to(columns[p, k][k : k + 1, :], (8, 128))
            pivot_row = jnp.broadcast_to(rows[p][k : k + 1, :], (8, 128))
            entries = [
                jnp.broadcast_to(columns[p, later][k : k + 1, :], (8, 128))
                for later in range(k + 1, 8)
            ]
            for t in range(p, 8):
                factor = columns[t, k] * inverse
                if t == p:
                    factor = jnp.where(below > k, factor, 0.0)
                rows[t] = rows[t] - factor * pivot_row
                for later in range(k + 1, 8):
                    columns[t, later] = columns[t, later] - factor * entries[later - k - 1]
    return jnp.concatenate(rows, axis=0)


def factor_inverse(gram_ref, inverse_ref, work_ref):
    size = gram_ref.shape[0]
    work_ref[...] = gram_ref[...]
    row = lax.broadcasted_iota(jnp.int32, (size, size), 0)
    column = lax.broadcasted_iota(jnp.int32, (size, size), 1)
    inverse_ref[...] = jnp.where(row == column, 1.0, 0.0).astype(jnp.float32)
    lane = lax.broadcasted_iota(jnp.int32, (BLOCK, 128), 1)
    line = lax.broadcasted_iota(jnp.int32, (BLOCK, 128), 0)
    for start in range(0, size, BLOCK):
        own = slice(start, start + BLOCK)
        tile_start = start // 128 * 128
        tile = work_ref[own, tile_start : tile_start + 128]
        if start % 128:
            tile = pltpu.roll(tile, 64, 1)
        unit = jnp.where(lane - BLOCK == line, 1.0, 0.0)
        done = eliminate(jnp.where(lane < BLOCK, tile, unit))
        pivots = jnp.sum(jnp.where(lane == line, done, 0.0), axis=1, keepdims=True)
        scaled = pltpu.roll(done * lax.rsqrt(pivots), 64, 1)[:, :BLOCK]
        left = jnp.dot(scaled, work_ref[own, :], precision=HIGHEST, preferred_element_type=jnp.float32)
        right = jnp.dot(scaled, inverse_ref[own, :], precision=HIGHEST, preferred_element_type=jnp.float32)
        inverse_ref[own, :] = right
        rest = size - start - BLOCK
        if rest:
            lower = slice(start + BLOCK, size)
            flipped = left.T[start + BLOCK :, :]
            work_ref[lower, :] -= jnp.dot(flipped, left, precision=HIGHEST, preferred_element_type=jnp.float32)
            inverse_ref[lower, :] -= jnp.dot(flipped, right, precision=HIGHEST, preferred_element_type=jnp.float32)


MESH_ID = pl.DeviceIdType.MESH


def greet(peers):
    barrier = pltpu.get_barrier_semaphore()
    for peer in peers:
        pl.semaphore_signal(barrier, inc=1, device_id=peer, device_id_type=MESH_ID)
    pl.semaphore_wait(barrier, len(peers))


def sketch_and_gram(
    n_texel, n_light, tex_ref, feat_ref, sketch_ref, counts_ref, basis_ref, coeffs_ref,
    tile_ref, inverse_ref, half_ref, product_ref, held, arrived,
    logits, partial_ref,
    landed, whole, pieces, plane, column, gram, scaled, work,
    part_send, part_recv, plane_send, plane_recv, column_send, column_recv,
    full_send, full_recv, row_send, row_recv, out_send, out_recv,
):
    texel, light = lax.axis_index("texel"), lax.axis_index("light")
    depth = partial_ref.shape[0] // n_light
    size = partial_ref.shape[1]
    piece = size // n_texel
    own_count = counts_ref[texel]
    valid = counts_ref[0]
    for index in range(1, n_texel):
        valid = valid + counts_ref[index]
    valid = valid.astype(jnp.float32)
    lights = [lax.rem(light + d, n_light) for d in range(n_light)]
    texels = [lax.rem(texel + d, n_texel) for d in range(n_texel)]
    greet([(texel, lights[d]) for d in range(1, n_light)] + [(texels[d], light) for d in range(1, n_texel)])

    def send(source, target, send_sem, recv_sem, device):
        copy = pltpu.make_async_remote_copy(
            src_ref=source, dst_ref=target, send_sem=send_sem, recv_sem=recv_sem,
            device_id=device, device_id_type=MESH_ID,
        )
        copy.start()
        return copy

    def rows_of(index, height):
        return pl.ds(pl.multiple_of(index * height, height), height)

    step = logits.shape[1]

    def fill(index):
        texels_here = tex_ref[rows_of(index, depth), :]

        def block(c, carry):
            columns = rows_of(c, step)
            logits[...] = lax.dot_general(
                texels_here, feat_ref[columns, :], (((1,), (1,)), ((), ())), preferred_element_type=jnp.float32
            )

            def strip(i, inner):
                value = bounded_sine(logits[rows_of(i, 16), :]).astype(jnp.bfloat16)
                tile_ref[pl.ds(pl.multiple_of(index * depth + i * 16, 16), 16), columns] = value
                return inner

            return lax.fori_loop(0, depth // 16, strip, carry, unroll=2)

        lax.fori_loop(0, feat_ref.shape[0] // step, block, 0)
        rows = rows_of(index, depth)
        slot = index * depth + lax.broadcasted_iota(jnp.int32, (depth, size), 0)
        product = jnp.dot(tile_ref[rows, :], sketch_ref[...], preferred_element_type=jnp.float32)
        partial_ref[rows, :] = jnp.where(slot < own_count, product, 0.0)

    copies = []
    for d in range(1, n_light):
        fill(lights[d])
        copies.append(
            send(
                partial_ref.at[rows_of(lights[d], depth)], landed.at[d],
                part_send.at[d], part_recv.at[d], (texel, lights[d]),
            )
        )
    fill(light)
    own = partial_ref[rows_of(light, depth), :]
    for d, copy in enumerate(copies, 1):
        copy.wait()
        own = own + landed[d]
    whole[rows_of(light, depth), :] = own
    early = depth // 4

    def gather(part, first, height):
        rows = pl.ds(pl.multiple_of(light * depth + first, 8), height)
        return [
            send(
                whole.at[rows], whole.at[rows], full_send.at[part, d], full_recv.at[part, d], (texel, lights[d])
            )
            for d in range(1, n_light)
        ]

    gathers = gather(0, 0, early)
    local = lax.dot_general(
        own, own, (((0,), (0,)), ((), ())), precision=HIGHEST, preferred_element_type=jnp.float32
    )
    for index in range(n_texel):
        pieces[index] = local[index * piece : (index + 1) * piece, :]
    copies = [
        send(pieces.at[texels[d]], plane.at[d], plane_send.at[d], plane_recv.at[d], (texels[d], light))
        for d in range(1, n_texel)
    ]
    total = pieces[texel]
    for d, copy in enumerate(copies, 1):
        copy.wait()
        total = total + plane[d]
    column[light] = total
    copies = [
        send(column.at[light], column.at[light], column_send.at[d], column_recv.at[d], (texel, lights[d]))
        for d in range(1, n_light)
    ]
    for copy in copies:
        copy.wait()
    gathers += gather(1, early, depth - early)
    total = column[0]
    for index in range(1, n_light):
        total = total + column[index]
    gram[rows_of(texel, piece), :] = total
    copies = [
        send(
            gram.at[rows_of(texel, piece)], gram.at[rows_of(texel, piece)],
            row_send.at[d], row_recv.at[d], (texels[d], light),
        )
        for d in range(1, n_texel)
    ]
    for copy in copies:
        copy.wait()
    scaled[...] = gram[...] / valid
    factor_inverse(scaled, inverse_ref, work)
    for copy in gathers:
        copy.wait()
    for index in range(n_light):
        rows = slice(index * depth, (index + 1) * depth)
        basis = lax.dot_general(
            whole[rows, :], inverse_ref[...], (((1,), (1,)), ((), ())), precision=HIGHEST,
            preferred_element_type=jnp.float32,
        )
        basis_ref[rows, :] = basis
        half_ref[rows, :] = basis.astype(jnp.bfloat16)
    scatter_sum(
        n_texel, half_ref, tile_ref, product_ref, coeffs_ref, valid, held, arrived, out_send, out_recv
    )


def halving_order(bits, last_first):
    rest = list(range(1, bits))
    return [0] + (rest[::-1] if last_first else rest)


def scatter_sum(n_texel, half_ref, tile_ref, partial_ref, out_ref, valid, held, landed, send_sem, recv_sem):
    texel, light = lax.axis_index("texel"), lax.axis_index("light")
    bits = n_texel.bit_length() - 1
    bit = [lax.rem(texel // (1 << b), 2) for b in range(bits)]
    partner = [texel + (1 - 2 * bit[b]) * (1 << b) for b in range(bits)]
    piece = partial_ref.shape[0] // n_texel
    width = partial_ref.shape[1] // 2

    def start_of(mask):
        block = 0
        for b in range(bits):
            flipped = 1 - bit[b] if mask >> b & 1 else bit[b]
            block = block + flipped * (1 << b)
        return pl.multiple_of(block * piece, piece)

    def multiply(half):
        columns = slice(half * width, (half + 1) * width)
        partial_ref[:, columns] = lax.dot_general(
            half_ref[...], tile_ref[:, columns], (((0,), (0,)), ((), ())), preferred_element_type=jnp.float32
        )

    orders = [halving_order(bits, False), halving_order(bits, True)]
    root = jnp.sqrt(jnp.full((piece, width), valid))
    flights = [{}, {}]
    for step in range(bits):
        for half, order in enumerate(orders):
            if step == 0:
                multiply(half)
            b = order[step]
            left = [m for m in range(n_texel) if all(not m >> done & 1 for done in order[:step])]
            later = order[step + 1 :]
            going = [m for m in left if m >> b & 1]
            going.sort(key=lambda m: [-(m >> c & 1) for c in later])
            columns = pl.ds(half * width, width)
            for m in going:
                kept = m - (1 << b)
                if step == 0:
                    source = partial_ref.at[pl.ds(start_of(m), piece), columns]
                else:
                    arrived = flights[half].pop((step - 1, m))
                    arrived.wait()
                    below = (
                        partial_ref[pl.ds(start_of(m), piece), columns] if step == 1 else held[half, m]
                    )
                    held[half, m] = below + landed[half, step - 1, m]
                    source = held.at[half, m]
                copy = pltpu.make_async_remote_copy(
                    src_ref=source,
                    dst_ref=landed.at[half, step, kept],
                    send_sem=send_sem.at[half, step, kept],
                    recv_sem=recv_sem.at[half, step, kept],
                    device_id=(partner[b], light),
                    device_id_type=MESH_ID,
                )
                copy.start()
                flights[half][step, kept] = copy
        if step:
            for half, order in enumerate(orders):
                for key in [k for k in flights[half] if k[0] == step - 1]:
                    m = key[1]
                    flights[half].pop(key).wait()
                    columns = pl.ds(half * width, width)
                    below = (
                        partial_ref[pl.ds(start_of(m), piece), columns] if step == 1 else held[half, m]
                    )
                    held[half, m] = below + landed[half, step - 1, m]
    for half in range(2):
        columns = pl.ds(half * width, width)
        flights[half].pop((bits - 1, 0)).wait()
        below = partial_ref[pl.ds(start_of(0), piece), columns] if bits == 1 else held[half, 0]
        out_ref[:, half * width : (half + 1) * width] = (below + landed[half, bits - 1, 0]) / root


def on_device(n_texel, n_light, tex_feat, light_feat, sketch, row_counts):
    capacity, size = tex_feat.shape[0], sketch.shape[1]
    lights = light_feat.shape[0]
    step = next(w for w in (512, 256, 128) if lights % w == 0)
    depth, piece = capacity // n_light, size // n_texel
    width, bits = lights // 2, n_texel.bit_length() - 1
    vmem = pl.BlockSpec(memory_space=pltpu.VMEM)
    smem = pl.BlockSpec(memory_space=pltpu.SMEM)
    f32, half = jnp.float32, jnp.bfloat16
    sems = pltpu.SemaphoreType.DMA
    return pl.pallas_call(
        functools.partial(sketch_and_gram, n_texel, n_light),
        out_shape=(
            jax.ShapeDtypeStruct((capacity, size), f32),
            jax.ShapeDtypeStruct((piece, lights), f32),
        ),
        in_specs=[vmem] * 3 + [smem],
        out_specs=(vmem, vmem),
        scratch_shapes=[
            pltpu.VMEM((capacity, lights), half),
            pltpu.VMEM((size, size), f32),
            pltpu.VMEM((capacity, size), half),
            pltpu.VMEM((size, lights), f32),
            pltpu.VMEM((2, n_texel, piece, width), f32),
            pltpu.VMEM((2, bits, n_texel, piece, width), f32),
            pltpu.VMEM((depth, step), f32),
            pltpu.VMEM((capacity, size), f32),
            pltpu.VMEM((n_light, depth, size), f32),
            pltpu.VMEM((capacity, size), f32),
            pltpu.VMEM((n_texel, piece, size), f32),
            pltpu.VMEM((n_texel, piece, size), f32),
            pltpu.VMEM((n_light, piece, size), f32),
            pltpu.VMEM((size, size), f32),
            pltpu.VMEM((size, size), f32),
            pltpu.VMEM((size, size), f32),
            sems((n_light,)), sems((n_light,)),
            sems((n_texel,)), sems((n_texel,)),
            sems((n_light,)), sems((n_light,)),
            sems((2, n_light)), sems((2, n_light)),
            sems((n_texel,)), sems((n_texel,)),
            sems((2, bits, n_texel)), sems((2, bits, n_texel)),
        ],
        compiler_params=pltpu.CompilerParams(collective_id=1, has_side_effects=True),
    )(tex_feat, light_feat, sketch, row_counts)


def solution(mesh):
    placed = (P("texel", None), P("light", None), P("light", None), P())
    return jax.shard_map(
        functools.partial(on_device, mesh.shape["texel"], mesh.shape["light"]),
        mesh=mesh,
        in_specs=placed,
        out_specs=(P("texel", None), P("texel", "light")),
        check_vma=False,
    )
```

```python
import functools

import jax
import jax.numpy as jnp
from jax import lax
from jax.experimental import pallas as pl
from jax.experimental.pallas import tpu as pltpu
from jax.sharding import PartitionSpec as P

HIGHEST = lax.Precision.HIGHEST
BLOCK = 64
CHUNK = 32
INV_TWO_PI = 0.15915494309189535
SINE = (6.283185273788226, -41.34167747777608, 81.60223120329199, -76.57499125549666, 39.71091094809089)


def bounded_sine(x):
    turns = x * INV_TWO_PI - 0.25
    z = 0.25 - jnp.abs(turns - jnp.round(turns))
    s = z * z
    value = SINE[-1] * s + SINE[-2]
    for coefficient in SINE[-3::-1]:
        value = value * s + coefficient
    return value * z


def eliminate(block):
    rows = [block[8 * t : 8 * t + 8, :] for t in range(8)]
    below = lax.broadcasted_iota(jnp.int32, (8, 128), 0)
    for p in range(8):
        columns = {
            (t, k): jnp.broadcast_to(rows[t][:, 8 * p + k : 8 * p + k + 1], (8, 128))
            for t in range(p, 8)
            for k in range(8)
        }
        for k in range(8):
            inverse = 1.0 / jnp.broadcast_to(columns[p, k][k : k + 1, :], (8, 128))
            pivot_row = jnp.broadcast_to(rows[p][k : k + 1, :], (8, 128))
            entries = [
                jnp.broadcast_to(columns[p, later][k : k + 1, :], (8, 128))
                for later in range(k + 1, 8)
            ]
            for t in range(p, 8):
                factor = columns[t, k] * inverse
                if t == p:
                    factor = jnp.where(below > k, factor, 0.0)
                rows[t] = rows[t] - factor * pivot_row
                for later in range(k + 1, 8):
                    columns[t, later] = columns[t, later] - factor * entries[later - k - 1]
    return jnp.concatenate(rows, axis=0)


def factor_inverse(gram_ref, inverse_ref, work_ref):
    size = gram_ref.shape[0]
    work_ref[...] = gram_ref[...]
    row = lax.broadcasted_iota(jnp.int32, (size, size), 0)
    column = lax.broadcasted_iota(jnp.int32, (size, size), 1)
    inverse_ref[...] = jnp.where(row == column, 1.0, 0.0).astype(jnp.float32)
    lane = lax.broadcasted_iota(jnp.int32, (BLOCK, 128), 1)
    line = lax.broadcasted_iota(jnp.int32, (BLOCK, 128), 0)
    for start in range(0, size, BLOCK):
        own = slice(start, start + BLOCK)
        tile_start = start // 128 * 128
        tile = work_ref[own, tile_start : tile_start + 128]
        if start % 128:
            tile = pltpu.roll(tile, 64, 1)
        unit = jnp.where(lane - BLOCK == line, 1.0, 0.0)
        done = eliminate(jnp.where(lane < BLOCK, tile, unit))
        pivots = jnp.sum(jnp.where(lane == line, done, 0.0), axis=1, keepdims=True)
        scaled = pltpu.roll(done * lax.rsqrt(pivots), 64, 1)[:, :BLOCK]
        left = jnp.dot(scaled, work_ref[own, :], precision=HIGHEST, preferred_element_type=jnp.float32)
        right = jnp.dot(scaled, inverse_ref[own, :], precision=HIGHEST, preferred_element_type=jnp.float32)
        inverse_ref[own, :] = right
        rest = size - start - BLOCK
        if rest:
            lower = slice(start + BLOCK, size)
            flipped = left.T[start + BLOCK :, :]
            work_ref[lower, :] -= jnp.dot(flipped, left, precision=HIGHEST, preferred_element_type=jnp.float32)
            inverse_ref[lower, :] -= jnp.dot(flipped, right, precision=HIGHEST, preferred_element_type=jnp.float32)


MESH_ID = pl.DeviceIdType.MESH


def relay_order(chunks):
    hop = 0.29 * chunks
    events = [(c, "inward", c) for c in range(chunks)]
    events += [(c + hop, "outward", c) for c in range(chunks)]
    events += [(c + 3 * hop, "back_inward", c) for c in range(chunks)]
    events += [(c + 4 * hop, "back_outward", c) for c in range(chunks)]
    return [(kind, c) for _, kind, c in sorted(events)]


def whole_step(
    n_texel, n_light, tex_ref, feat_ref, sketch_ref, counts_ref, basis_ref, coeffs_ref,
    tile_ref, inverse_ref, half_ref, product_ref, held, arrived,
    logits_even, logits_odd, partial_ref,
    landed, whole, pieces, plane, column, gram, scaled, work,
    sum_send, sum_recv, back_send, back_recv, plane_send, plane_recv, column_send, column_recv,
    row_send, row_recv, out_send, out_recv,
):
    texel, light = lax.axis_index("texel"), lax.axis_index("light")
    capacity, size = partial_ref.shape
    width = logits_even.shape[1]
    block = logits_even.shape[0]
    middle = capacity // 2
    chunks = middle // CHUNK
    piece = size // n_texel
    own_count = counts_ref[texel]
    valid = counts_ref[0]
    for index in range(1, n_texel):
        valid = valid + counts_ref[index]
    valid = valid.astype(jnp.float32)
    lights = [lax.rem(light + d, n_light) for d in range(n_light)]
    texels = [lax.rem(texel + d, n_texel) for d in range(n_texel)]
    upper = light // (n_light // 2)
    inward, outward = 1 - upper, upper
    depth = light + upper * (n_light - 1 - 2 * light)
    toward_middle = light + 1 - 2 * upper
    toward_end = light - 1 + 2 * upper

    barrier = pltpu.get_barrier_semaphore()
    peers = [(texel, lights[d]) for d in range(1, n_light)] + [(texels[d], light) for d in range(1, n_texel)]
    for peer in peers:
        pl.semaphore_signal(barrier, inc=1, device_id=peer, device_id_type=MESH_ID)

    def copy(source, target, send_sem, recv_sem, device):
        return pltpu.make_async_remote_copy(
            src_ref=source, dst_ref=target, send_sem=send_sem, recv_sem=recv_sem,
            device_id=device, device_id_type=MESH_ID,
        )

    def rows_of(index, height):
        return pl.ds(pl.multiple_of(index * height, height), height)

    def chunk_rows(half, c):
        return pl.ds(pl.multiple_of(half * middle + c * CHUNK, CHUNK), CHUNK)

    def sum_copy(half, c, to):
        return copy(
            partial_ref.at[chunk_rows(half, c)], landed.at[half, c],
            sum_send.at[half, c], sum_recv.at[half, c], (texel, to),
        )

    def back_copy(half, c, to):
        rows = chunk_rows(half, c)
        return copy(
            whole.at[rows], whole.at[rows], back_send.at[half, c], back_recv.at[half, c], (texel, to)
        )

    def fill(first):
        rows = pl.ds(pl.multiple_of(first, block), block)
        logits = (logits_even, logits_odd)
        count = feat_ref.shape[0] // width

        def product_of(c):
            return lax.dot_general(
                tex_ref[rows, :], feat_ref[c * width : (c + 1) * width, :], (((1,), (1,)), ((), ())),
                preferred_element_type=jnp.float32,
            )

        logits[0][...] = product_of(0)
        for c in range(count):
            if c + 1 < count:
                logits[(c + 1) % 2][...] = product_of(c + 1)
            tile_ref[rows, c * width : (c + 1) * width] = bounded_sine(logits[c % 2][...]).astype(jnp.bfloat16)
        slot = first + lax.broadcasted_iota(jnp.int32, (block, size), 0)
        product = jnp.dot(tile_ref[rows, :], sketch_ref[...], preferred_element_type=jnp.float32)
        partial_ref[rows, :] = jnp.where(slot < own_count, product, 0.0)

    blocks = middle // block
    per_block = block // CHUNK
    for b in range(blocks):
        fill(inward * middle + b * block)
        if b == 0:
            pl.semaphore_wait(barrier, len(peers))

        @pl.when(depth == 0)
        def _():
            for c in range(b * per_block, (b + 1) * per_block):
                sum_copy(inward, c, toward_middle).start()

    for b in range(blocks):
        fill(outward * middle + b * block)

    @pl.when(depth == 0)
    def _():
        for c in range(chunks):
            sum_copy(outward, c, toward_middle).wait_recv()
            rows = chunk_rows(outward, c)
            whole[rows, :] = partial_ref[rows, :] + landed[outward, c]
            if c == 0:
                for sent in range(chunks):
                    sum_copy(inward, sent, toward_middle).wait_send()
            back_copy(outward, c, toward_middle).start()
        own = whole[pl.ds(pl.multiple_of(outward * middle, middle), middle), :]
        local = lax.dot_general(
            own, own, (((0,), (0,)), ((), ())), precision=HIGHEST, preferred_element_type=jnp.float32
        )
        for index in range(n_texel):
            pieces[index] = local[index * piece : (index + 1) * piece, :]
        copies = [
            copy(pieces.at[texels[d]], plane.at[d], plane_send.at[d], plane_recv.at[d], (texels[d], light))
            for d in range(1, n_texel)
        ]
        for going in copies:
            going.start()
        total = pieces[texel]
        for d, going in enumerate(copies, 1):
            going.wait()
            total = total + plane[d]
        column[upper] = total
        for d in range(1, n_light):
            copy(
                column.at[upper], column.at[upper], column_send.at[d], column_recv.at[upper], (texel, lights[d])
            ).start()

    @pl.when(depth > 0)
    def _():
        for kind, c in relay_order(chunks):
            if kind == "inward" or kind == "outward":
                half, to = (inward, toward_middle) if kind == "inward" else (outward, toward_end)
                going = sum_copy(half, c, to)
                going.wait_recv()
                rows = chunk_rows(half, c)
                partial_ref[rows, :] = partial_ref[rows, :] + landed[half, c]
                going.start()
            else:
                half, to = (outward, toward_middle) if kind == "back_inward" else (inward, toward_end)
                going = back_copy(half, c, to)
                going.wait_recv()
                going.start()
        copy(column.at[upper], column.at[upper], column_send.at[0], column_recv.at[upper], (texel, lights[1])).wait_recv()

    other = 1 - upper
    copy(column.at[other], column.at[other], column_send.at[0], column_recv.at[other], (texel, lights[1])).wait_recv()
    gram[rows_of(texel, piece), :] = column[0] + column[1]
    copies = [
        copy(
            gram.at[rows_of(texel, piece)], gram.at[rows_of(texel, piece)],
            row_send.at[d], row_recv.at[d], (texels[d], light),
        )
        for d in range(1, n_texel)
    ]
    for going in copies:
        going.start()
    for going in copies:
        going.wait()
    scaled[...] = gram[...] / valid
    factor_inverse(scaled, inverse_ref, work)

    @pl.when(depth == 0)
    def _():
        for c in range(chunks):
            back_copy(inward, c, toward_middle).wait_recv()
            back_copy(outward, c, toward_middle).wait_send()
        for d in range(1, n_light):
            copy(
                column.at[upper], column.at[upper], column_send.at[d], column_recv.at[upper], (texel, lights[d])
            ).wait_send()

    @pl.when(depth > 0)
    def _():
        for c in range(chunks):
            sum_copy(inward, c, toward_middle).wait_send()
            sum_copy(outward, c, toward_end).wait_send()
            back_copy(outward, c, toward_middle).wait_send()
            back_copy(inward, c, toward_end).wait_send()

    for index in range(capacity // block):
        rows = slice(index * block, (index + 1) * block)
        basis = lax.dot_general(
            whole[rows, :], inverse_ref[...], (((1,), (1,)), ((), ())), precision=HIGHEST,
            preferred_element_type=jnp.float32,
        )
        basis_ref[rows, :] = basis
        half_ref[rows, :] = basis.astype(jnp.bfloat16)
    scatter_sum(
        n_texel, half_ref, tile_ref, product_ref, coeffs_ref, valid, held, arrived, out_send, out_recv
    )


def halving_order(bits, last_first):
    rest = list(range(1, bits))
    return [0] + (rest[::-1] if last_first else rest)


def scatter_sum(n_texel, half_ref, tile_ref, partial_ref, out_ref, valid, held, landed, send_sem, recv_sem):
    texel, light = lax.axis_index("texel"), lax.axis_index("light")
    bits = n_texel.bit_length() - 1
    bit = [lax.rem(texel // (1 << b), 2) for b in range(bits)]
    partner = [texel + (1 - 2 * bit[b]) * (1 << b) for b in range(bits)]
    piece = partial_ref.shape[0] // n_texel
    width = partial_ref.shape[1] // 2

    def start_of(mask):
        block = 0
        for b in range(bits):
            flipped = 1 - bit[b] if mask >> b & 1 else bit[b]
            block = block + flipped * (1 << b)
        return pl.multiple_of(block * piece, piece)

    def multiply(half):
        columns = slice(half * width, (half + 1) * width)
        partial_ref[:, columns] = lax.dot_general(
            half_ref[...], tile_ref[:, columns], (((0,), (0,)), ((), ())), preferred_element_type=jnp.float32
        )

    orders = [halving_order(bits, False), halving_order(bits, True)]
    root = jnp.sqrt(jnp.full((piece, width), valid))
    flights = [{}, {}]
    for step in range(bits):
        for half, order in enumerate(orders):
            if step == 0:
                multiply(half)
            b = order[step]
            left = [m for m in range(n_texel) if all(not m >> done & 1 for done in order[:step])]
            later = order[step + 1 :]
            going = [m for m in left if m >> b & 1]
            going.sort(key=lambda m: [-(m >> c & 1) for c in later])
            columns = pl.ds(half * width, width)
            for m in going:
                kept = m - (1 << b)
                if step == 0:
                    source = partial_ref.at[pl.ds(start_of(m), piece), columns]
                else:
                    arrived = flights[half].pop((step - 1, m))
                    arrived.wait()
                    below = (
                        partial_ref[pl.ds(start_of(m), piece), columns] if step == 1 else held[half, m]
                    )
                    held[half, m] = below + landed[half, step - 1, m]
                    source = held.at[half, m]
                copy = pltpu.make_async_remote_copy(
                    src_ref=source,
                    dst_ref=landed.at[half, step, kept],
                    send_sem=send_sem.at[half, step, kept],
                    recv_sem=recv_sem.at[half, step, kept],
                    device_id=(partner[b], light),
                    device_id_type=MESH_ID,
                )
                copy.start()
                flights[half][step, kept] = copy
        if step:
            for half, order in enumerate(orders):
                for key in [k for k in flights[half] if k[0] == step - 1]:
                    m = key[1]
                    flights[half].pop(key).wait()
                    columns = pl.ds(half * width, width)
                    below = (
                        partial_ref[pl.ds(start_of(m), piece), columns] if step == 1 else held[half, m]
                    )
                    held[half, m] = below + landed[half, step - 1, m]
    for half in range(2):
        columns = pl.ds(half * width, width)
        flights[half].pop((bits - 1, 0)).wait()
        below = partial_ref[pl.ds(start_of(0), piece), columns] if bits == 1 else held[half, 0]
        out_ref[:, half * width : (half + 1) * width] = (below + landed[half, bits - 1, 0]) / root


def write_out(basis_ref, coeffs_ref, basis_out, coeffs_out, sems):
    copies = [
        pltpu.make_async_copy(basis_ref, basis_out, sems.at[0]),
        pltpu.make_async_copy(coeffs_ref, coeffs_out, sems.at[1]),
    ]
    for going in copies:
        going.start()
    for going in copies:
        going.wait()


def on_device(n_texel, n_light, tex_feat, light_feat, sketch, row_counts):
    capacity, size = tex_feat.shape[0], sketch.shape[1]
    lights = light_feat.shape[0]
    block, step = capacity // 4, next(w for w in (256, 128) if lights % w == 0)
    chunks, piece = capacity // 2 // CHUNK, size // n_texel
    width, bits = lights // 2, n_texel.bit_length() - 1
    vmem = pl.BlockSpec(memory_space=pltpu.VMEM)
    smem = pl.BlockSpec(memory_space=pltpu.SMEM)
    f32, half = jnp.float32, jnp.bfloat16
    sems = pltpu.SemaphoreType.DMA
    basis, coeffs = pl.pallas_call(
        functools.partial(whole_step, n_texel, n_light),
        out_shape=(pltpu.VMEM((capacity, size), f32), pltpu.VMEM((piece, lights), f32)),
        in_specs=[vmem] * 3 + [smem],
        out_specs=(vmem, vmem),
        scratch_shapes=[
            pltpu.VMEM((capacity, lights), half),
            pltpu.VMEM((size, size), f32),
            pltpu.VMEM((capacity, size), half),
            pltpu.VMEM((size, lights), f32),
            pltpu.VMEM((2, n_texel, piece, width), f32),
            pltpu.VMEM((2, bits, n_texel, piece, width), f32),
            pltpu.VMEM((block, step), f32),
            pltpu.VMEM((block, step), f32),
            pltpu.VMEM((capacity, size), f32),
            pltpu.VMEM((2, chunks, CHUNK, size), f32),
            pltpu.VMEM((capacity, size), f32),
            pltpu.VMEM((n_texel, piece, size), f32),
            pltpu.VMEM((n_texel, piece, size), f32),
            pltpu.VMEM((2, piece, size), f32),
            pltpu.VMEM((size, size), f32),
            pltpu.VMEM((size, size), f32),
            pltpu.VMEM((size, size), f32),
            sems((2, chunks)), sems((2, chunks)),
            sems((2, chunks)), sems((2, chunks)),
            sems((n_texel,)), sems((n_texel,)),
            sems((n_light,)), sems((2,)),
            sems((n_texel,)), sems((n_texel,)),
            sems((2, bits, n_texel)), sems((2, bits, n_texel)),
        ],
        compiler_params=pltpu.CompilerParams(collective_id=1, has_side_effects=True),
    )(tex_feat, light_feat, sketch, row_counts)
    return pl.pallas_call(
        write_out,
        out_shape=(jax.ShapeDtypeStruct((capacity, size), f32), jax.ShapeDtypeStruct((piece, lights), f32)),
        in_specs=[vmem, vmem],
        out_specs=(pl.BlockSpec(memory_space=pl.ANY),) * 2,
        scratch_shapes=[sems((2,))],
    )(*(pltpu.with_memory_space_constraint(x, pltpu.VMEM) for x in (basis, coeffs)))


def solution(mesh):
    placed = (P("texel", None), P("light", None), P("light", None), P())
    return jax.shard_map(
        functools.partial(on_device, mesh.shape["texel"], mesh.shape["light"]),
        mesh=mesh,
        in_specs=placed,
        out_specs=(P("texel", None), P("texel", "light")),
        check_vma=False,
    )
```

```python
import functools

import jax
import jax.numpy as jnp
from jax import lax
from jax.experimental import pallas as pl
from jax.experimental.pallas import tpu as pltpu
from jax.sharding import PartitionSpec as P

HIGHEST = lax.Precision.HIGHEST
BLOCK = 64
CHUNK = 32
INV_TWO_PI = 0.15915494309189535
SINE = (6.283185273788226, -41.34167747777608, 81.60223120329199, -76.57499125549666, 39.71091094809089)


def bounded_sine(x):
    turns = x * INV_TWO_PI - 0.25
    z = 0.25 - jnp.abs(turns - jnp.round(turns))
    s = z * z
    value = SINE[-1] * s + SINE[-2]
    for coefficient in SINE[-3::-1]:
        value = value * s + coefficient
    return value * z


def eliminate(block):
    rows = [block[8 * t : 8 * t + 8, :] for t in range(8)]
    below = lax.broadcasted_iota(jnp.int32, (8, 128), 0)
    for p in range(8):
        columns = {
            (t, k): jnp.broadcast_to(rows[t][:, 8 * p + k : 8 * p + k + 1], (8, 128))
            for t in range(p, 8)
            for k in range(8)
        }
        for k in range(8):
            inverse = 1.0 / jnp.broadcast_to(columns[p, k][k : k + 1, :], (8, 128))
            pivot_row = jnp.broadcast_to(rows[p][k : k + 1, :], (8, 128))
            entries = [
                jnp.broadcast_to(columns[p, later][k : k + 1, :], (8, 128))
                for later in range(k + 1, 8)
            ]
            for t in range(p, 8):
                factor = columns[t, k] * inverse
                if t == p:
                    factor = jnp.where(below > k, factor, 0.0)
                rows[t] = rows[t] - factor * pivot_row
                for later in range(k + 1, 8):
                    columns[t, later] = columns[t, later] - factor * entries[later - k - 1]
    return jnp.concatenate(rows, axis=0)


def factor_inverse(work_ref, inverse_ref, finish_gram):
    size = work_ref.shape[0]
    row = lax.broadcasted_iota(jnp.int32, (size, size), 0)
    column = lax.broadcasted_iota(jnp.int32, (size, size), 1)
    inverse_ref[...] = jnp.where(row == column, 1.0, 0.0).astype(jnp.float32)
    lane = lax.broadcasted_iota(jnp.int32, (BLOCK, 128), 1)
    line = lax.broadcasted_iota(jnp.int32, (BLOCK, 128), 0)
    for start in range(0, size, BLOCK):
        own = slice(start, start + BLOCK)
        tile_start = start // 128 * 128
        tile = work_ref[own, tile_start : tile_start + 128]
        if start % 128:
            tile = pltpu.roll(tile, 64, 1)
        unit = jnp.where(lane - BLOCK == line, 1.0, 0.0)
        done = eliminate(jnp.where(lane < BLOCK, tile, unit))
        pivots = jnp.sum(jnp.where(lane == line, done, 0.0), axis=1, keepdims=True)
        scaled = pltpu.roll(done * lax.rsqrt(pivots), 64, 1)[:, :BLOCK]
        left = jnp.dot(scaled, work_ref[own, :], precision=HIGHEST, preferred_element_type=jnp.float32)
        right = jnp.dot(scaled, inverse_ref[own, :], precision=HIGHEST, preferred_element_type=jnp.float32)
        inverse_ref[own, :] = right
        if start == 0:
            finish_gram()
        rest = size - start - BLOCK
        if rest:
            lower = slice(start + BLOCK, size)
            flipped = left.T[start + BLOCK :, :]
            work_ref[lower, :] -= jnp.dot(flipped, left, precision=HIGHEST, preferred_element_type=jnp.float32)
            inverse_ref[lower, :] -= jnp.dot(flipped, right, precision=HIGHEST, preferred_element_type=jnp.float32)


MESH_ID = pl.DeviceIdType.MESH


def relay_order(chunks, relayed):
    hop = 0.29 * chunks
    events = [(c, "inward", c) for c in range(relayed)]
    events += [(c + hop, "outward", c) for c in range(relayed)]
    events += [(c + 3 * hop, "back_inward", c) for c in range(chunks)]
    events += [(c + 4 * hop, "back_outward", c) for c in range(chunks)]
    return [(kind, c) for _, kind, c in sorted(events)]


def whole_step(
    n_texel, n_light, tex_ref, feat_ref, sketch_ref, counts_ref, basis_ref, coeffs_ref,
    tile_ref, inverse_ref, half_ref, product_ref, held, arrived,
    logits_even, logits_odd, partial_ref,
    landed, straight, whole, work,
    pieces_first, pieces_rest, plane_first, plane_rest, column_first, column_rest, rows_first, rows_rest,
    sum_send, sum_recv, straight_send, straight_recv, back_send, back_recv,
    plane_send, plane_recv, column_send, column_recv, row_send, row_recv, out_send, out_recv,
):
    texel, light = lax.axis_index("texel"), lax.axis_index("light")
    capacity, size = partial_ref.shape
    width = logits_even.shape[1]
    block = logits_even.shape[0]
    middle = capacity // 2
    chunks = middle // CHUNK
    direct = straight.shape[2]
    relayed = chunks - direct
    own_count = counts_ref[texel]
    valid = counts_ref[0]
    for index in range(1, n_texel):
        valid = valid + counts_ref[index]
    valid = valid.astype(jnp.float32)
    lights = [lax.rem(light + d, n_light) for d in range(n_light)]
    texels = [lax.rem(texel + d, n_texel) for d in range(n_texel)]
    upper = light // (n_light // 2)
    inward, outward = 1 - upper, upper
    depth = light + upper * (n_light - 1 - 2 * light)
    inner = 1 - (n_light // 2 - depth) // (n_light // 2)
    toward_middle = light + 1 - 2 * upper
    toward_end = light - 1 + 2 * upper

    barrier = pltpu.get_barrier_semaphore()
    peers = [(texel, lights[d]) for d in range(1, n_light)] + [(texels[d], light) for d in range(1, n_texel)]
    for peer in peers:
        pl.semaphore_signal(barrier, inc=1, device_id=peer, device_id_type=MESH_ID)

    def copy(source, target, send_sem, recv_sem, device):
        return pltpu.make_async_remote_copy(
            src_ref=source, dst_ref=target, send_sem=send_sem, recv_sem=recv_sem,
            device_id=device, device_id_type=MESH_ID,
        )

    def chunk_rows(half, c):
        return pl.ds(pl.multiple_of(half * middle + c * CHUNK, CHUNK), CHUNK)

    def sum_copy(half, c, to):
        return copy(
            partial_ref.at[chunk_rows(half, c)], landed.at[half, c],
            sum_send.at[half, c], sum_recv.at[half, c], (texel, to),
        )

    def straight_copy(half, place, c, to):
        return copy(
            partial_ref.at[chunk_rows(half, relayed + c)], straight.at[half, place, c],
            straight_send.at[half, c], straight_recv.at[half, place, c], (texel, to),
        )

    def straight_own(half, c):
        place = half * light + (1 - half) * (n_light - 1 - light)
        return straight_copy(half, place, c, half * (n_light - 1))

    def back_copy(half, c, to):
        rows = chunk_rows(half, c)
        return copy(
            whole.at[rows], whole.at[rows], back_send.at[half, c], back_recv.at[half, c], (texel, to)
        )

    def fill(first):
        rows = pl.ds(pl.multiple_of(first, block), block)
        logits = (logits_even, logits_odd)
        count = feat_ref.shape[0] // width

        def product_of(c):
            return lax.dot_general(
                tex_ref[rows, :], feat_ref[c * width : (c + 1) * width, :], (((1,), (1,)), ((), ())),
                preferred_element_type=jnp.float32,
            )

        logits[0][...] = product_of(0)
        for c in range(count):
            if c + 1 < count:
                logits[(c + 1) % 2][...] = product_of(c + 1)
            tile_ref[rows, c * width : (c + 1) * width] = bounded_sine(logits[c % 2][...]).astype(jnp.bfloat16)
        slot = first + lax.broadcasted_iota(jnp.int32, (block, size), 0)
        product = jnp.dot(tile_ref[rows, :], sketch_ref[...], preferred_element_type=jnp.float32)
        partial_ref[rows, :] = jnp.where(slot < own_count, product, 0.0)

    blocks = middle // block
    per_block = block // CHUNK
    for turn in range(2 * blocks):
        edge_half, edge_block = turn // blocks, turn % blocks
        inner_half, inner_block = turn % 2, blocks - 1 - turn // 2
        is_outward = (1 - inner) * edge_half + inner * inner_half
        which = (1 - inner) * edge_block + inner * inner_block
        fill((inward * (1 - is_outward) + outward * is_outward) * middle + which * block)
        if turn == 0:
            pl.semaphore_wait(barrier, len(peers))

        @pl.when(inner == 0)
        def _():
            if edge_half == 0:
                for c in range(edge_block * per_block, (edge_block + 1) * per_block):
                    if c < relayed:
                        sum_copy(inward, c, toward_middle).start()
                    else:
                        straight_own(inward, c - relayed).start()

        @pl.when(inner == 1)
        def _():
            for c in range(inner_block * per_block, (inner_block + 1) * per_block):
                if c >= relayed:
                    straight_own(inward if inner_half == 0 else outward, c - relayed).start()

    groups = (
        (pieces_first, plane_first, column_first, rows_first),
        (pieces_rest, plane_rest, column_rest, rows_rest),
    )
    quarter = size // 4

    @pl.when(inner == 0)
    def _():
        for c in range(chunks):
            rows = chunk_rows(outward, c)
            if c < relayed:
                sum_copy(outward, c, toward_middle).wait_recv()
                whole[rows, :] = partial_ref[rows, :] + landed[outward, c]
            else:
                total = partial_ref[rows, :]
                for place in range(n_light - 1):
                    straight_copy(outward, place, c - relayed, toward_middle).wait_recv()
                    total = total + straight[outward, place, c - relayed]
                whole[rows, :] = total
            if c == 0:
                for sent in range(relayed):
                    sum_copy(inward, sent, toward_middle).wait_send()
                for sent in range(direct):
                    straight_own(inward, sent).wait_send()
            back_copy(outward, c, toward_middle).start()
        own = whole[pl.ds(pl.multiple_of(outward * middle, middle), middle), :]
        local = lax.dot_general(
            own, own, (((0,), (0,)), ((), ())), precision=HIGHEST, preferred_element_type=jnp.float32
        )
        rest = jnp.concatenate(
            [local[2 * quarter : 3 * quarter, 2 * quarter :], local[3 * quarter :, 2 * quarter :]], axis=1
        )
        rest = jnp.concatenate([local[quarter : 2 * quarter, :], rest], axis=0)
        for index in range(n_texel):
            for part, ref in ((local, pieces_first), (rest, pieces_rest)):
                height = ref.shape[1]
                ref[index] = part[index * height : (index + 1) * height, :]
        copies = [
            [
                copy(
                    pieces.at[texels[d]], plane.at[d], plane_send.at[g, d], plane_recv.at[g, d], (texels[d], light)
                )
                for d in range(1, n_texel)
            ]
            for g, (pieces, plane, _, _) in enumerate(groups)
        ]
        for going in copies[0] + copies[1]:
            going.start()
        for g, (pieces, plane, column, _) in enumerate(groups):
            total = pieces[texel]
            for d, going in enumerate(copies[g], 1):
                going.wait()
                total = total + plane[d]
            column[upper] = total
            for d in range(1, n_light):
                copy(
                    column.at[upper], column.at[upper], column_send.at[g, d], column_recv.at[g, upper],
                    (texel, lights[d]),
                ).start()

    def column_wait(g, side):
        column = groups[g][2]
        copy(
            column.at[side], column.at[side], column_send.at[g, 0], column_recv.at[g, side], (texel, lights[1])
        ).wait_recv()

    @pl.when(inner == 1)
    def _():
        for kind, c in relay_order(chunks, relayed):
            if kind == "inward" or kind == "outward":
                half, to = (inward, toward_middle) if kind == "inward" else (outward, toward_end)
                going = sum_copy(half, c, to)
                going.wait_recv()
                rows = chunk_rows(half, c)
                partial_ref[rows, :] = partial_ref[rows, :] + landed[half, c]
                going.start()
            else:
                half, to = (outward, toward_middle) if kind == "back_inward" else (inward, toward_end)
                going = back_copy(half, c, to)
                going.wait_recv()
                going.start()
        for g in range(2):
            column_wait(g, upper)

    row_copies = []
    for g, (_, _, column, rows) in enumerate(groups):
        column_wait(g, 1 - upper)
        rows[texel] = column[0] + column[1]
        row_copies.append(
            [
                copy(rows.at[texel], rows.at[texel], row_send.at[g, d], row_recv.at[g, texel], (texels[d], light))
                for d in range(1, n_texel)
            ]
        )
        for going in row_copies[g]:
            going.start()

    def row_wait(g):
        rows = groups[g][3]
        for d in range(1, n_texel):
            copy(
                rows.at[texels[d]], rows.at[texels[d]], row_send.at[g, d], row_recv.at[g, texels[d]], (texels[d], light)
            ).wait_recv()

    row_wait(0)
    height = rows_first.shape[1]
    for index in range(n_texel):
        work[index * height : (index + 1) * height, :] = rows_first[index] / valid

    def finish_gram():
        row_wait(1)
        height = rows_rest.shape[1]
        rest = jnp.concatenate([rows_rest[index] for index in range(n_texel)], axis=0) / valid
        work[quarter : 2 * quarter, :] = rest[:quarter, :]
        work[2 * quarter :, : 2 * quarter] = jnp.zeros((2 * quarter, 2 * quarter), jnp.float32)
        work[2 * quarter : 3 * quarter, 2 * quarter :] = rest[quarter:, : 2 * quarter]
        work[3 * quarter :, 2 * quarter :] = rest[quarter:, 2 * quarter :]

    factor_inverse(work, inverse_ref, finish_gram)

    @pl.when(inner == 0)
    def _():
        for c in range(chunks):
            back_copy(inward, c, toward_middle).wait_recv()
            back_copy(outward, c, toward_middle).wait_send()
        for g in range(2):
            column = groups[g][2]
            for d in range(1, n_light):
                copy(
                    column.at[upper], column.at[upper], column_send.at[g, d], column_recv.at[g, upper],
                    (texel, lights[d]),
                ).wait_send()

    @pl.when(inner == 1)
    def _():
        for c in range(chunks):
            if c < relayed:
                sum_copy(inward, c, toward_middle).wait_send()
                sum_copy(outward, c, toward_end).wait_send()
            else:
                straight_own(inward, c - relayed).wait_send()
                straight_own(outward, c - relayed).wait_send()
            back_copy(outward, c, toward_middle).wait_send()
            back_copy(inward, c, toward_end).wait_send()

    for going in row_copies[0] + row_copies[1]:
        going.wait_send()

    for index in range(capacity // block):
        rows = slice(index * block, (index + 1) * block)
        half_ref[:, rows] = lax.dot_general(
            inverse_ref[...], whole[rows, :], (((1,), (1,)), ((), ())), precision=HIGHEST,
            preferred_element_type=jnp.float32,
        ).astype(jnp.bfloat16)

    def basis_rows():
        for index in range(capacity // block):
            rows = slice(index * block, (index + 1) * block)
            basis_ref[rows, :] = lax.dot_general(
                whole[rows, :], inverse_ref[...], (((1,), (1,)), ((), ())), precision=HIGHEST,
                preferred_element_type=jnp.float32,
            )

    scatter_sum(
        n_texel, half_ref, tile_ref, product_ref, coeffs_ref, valid, held, arrived, out_send, out_recv, basis_rows
    )


def halving_order(bits, last_first):
    rest = list(range(1, bits))
    return [0] + (rest[::-1] if last_first else rest)


def scatter_sum(n_texel, half_ref, tile_ref, partial_ref, out_ref, valid, held, landed, send_sem, recv_sem, meanwhile):
    texel, light = lax.axis_index("texel"), lax.axis_index("light")
    bits = n_texel.bit_length() - 1
    bit = [lax.rem(texel // (1 << b), 2) for b in range(bits)]
    partner = [texel + (1 - 2 * bit[b]) * (1 << b) for b in range(bits)]
    piece = partial_ref.shape[0] // n_texel
    width = partial_ref.shape[1] // 2

    def start_of(mask):
        block = 0
        for b in range(bits):
            flipped = 1 - bit[b] if mask >> b & 1 else bit[b]
            block = block + flipped * (1 << b)
        return pl.multiple_of(block * piece, piece)

    def multiply(half):
        columns = slice(half * width, (half + 1) * width)
        partial_ref[:, columns] = lax.dot_general(
            half_ref[...], tile_ref[:, columns], (((1,), (0,)), ((), ())), preferred_element_type=jnp.float32
        )

    orders = [halving_order(bits, False), halving_order(bits, True)]
    root = jnp.sqrt(jnp.full((piece, width), valid))
    flights = [{}, {}]
    for step in range(bits):
        for half, order in enumerate(orders):
            if step == 0:
                multiply(half)
            b = order[step]
            left = [m for m in range(n_texel) if all(not m >> done & 1 for done in order[:step])]
            later = order[step + 1 :]
            going = [m for m in left if m >> b & 1]
            going.sort(key=lambda m: [-(m >> c & 1) for c in later])
            columns = pl.ds(half * width, width)
            for m in going:
                kept = m - (1 << b)
                if step == 0:
                    source = partial_ref.at[pl.ds(start_of(m), piece), columns]
                else:
                    arrived = flights[half].pop((step - 1, m))
                    arrived.wait()
                    below = (
                        partial_ref[pl.ds(start_of(m), piece), columns] if step == 1 else held[half, m]
                    )
                    held[half, m] = below + landed[half, step - 1, m]
                    source = held.at[half, m]
                copy = pltpu.make_async_remote_copy(
                    src_ref=source,
                    dst_ref=landed.at[half, step, kept],
                    send_sem=send_sem.at[half, step, kept],
                    recv_sem=recv_sem.at[half, step, kept],
                    device_id=(partner[b], light),
                    device_id_type=MESH_ID,
                )
                copy.start()
                flights[half][step, kept] = copy
        if step == 0:
            meanwhile()
        if step:
            for half, order in enumerate(orders):
                for key in [k for k in flights[half] if k[0] == step - 1]:
                    m = key[1]
                    flights[half].pop(key).wait()
                    columns = pl.ds(half * width, width)
                    below = (
                        partial_ref[pl.ds(start_of(m), piece), columns] if step == 1 else held[half, m]
                    )
                    held[half, m] = below + landed[half, step - 1, m]
    for half in range(2):
        columns = pl.ds(half * width, width)
        flights[half].pop((bits - 1, 0)).wait()
        below = partial_ref[pl.ds(start_of(0), piece), columns] if bits == 1 else held[half, 0]
        out_ref[:, half * width : (half + 1) * width] = (below + landed[half, bits - 1, 0]) / root


def write_out(basis_ref, coeffs_ref, basis_out, coeffs_out, sems):
    copies = [
        pltpu.make_async_copy(basis_ref, basis_out, sems.at[0]),
        pltpu.make_async_copy(coeffs_ref, coeffs_out, sems.at[1]),
    ]
    for going in copies:
        going.start()
    for going in copies:
        going.wait()


def on_device(n_texel, n_light, tex_feat, light_feat, sketch, row_counts):
    capacity, size = tex_feat.shape[0], sketch.shape[1]
    lights = light_feat.shape[0]
    block, step = capacity // 4, next(w for w in (256, 128) if lights % w == 0)
    chunks, piece = capacity // 2 // CHUNK, size // n_texel
    first, rest, direct = size // 4 // n_texel, size // 2 // n_texel, chunks // n_light
    width, bits = lights // 2, n_texel.bit_length() - 1
    vmem = pl.BlockSpec(memory_space=pltpu.VMEM)
    smem = pl.BlockSpec(memory_space=pltpu.SMEM)
    f32, half = jnp.float32, jnp.bfloat16
    sems = pltpu.SemaphoreType.DMA
    basis, coeffs = pl.pallas_call(
        functools.partial(whole_step, n_texel, n_light),
        out_shape=(pltpu.VMEM((capacity, size), f32), pltpu.VMEM((piece, lights), f32)),
        in_specs=[vmem] * 3 + [smem],
        out_specs=(vmem, vmem),
        scratch_shapes=[
            pltpu.VMEM((capacity, lights), half),
            pltpu.VMEM((size, size), f32),
            pltpu.VMEM((size, capacity), half),
            pltpu.VMEM((size, lights), f32),
            pltpu.VMEM((2, n_texel, piece, width), f32),
            pltpu.VMEM((2, bits, n_texel, piece, width), f32),
            pltpu.VMEM((block, step), f32),
            pltpu.VMEM((block, step), f32),
            pltpu.VMEM((capacity, size), f32),
            pltpu.VMEM((2, chunks, CHUNK, size), f32),
            pltpu.VMEM((2, n_light, direct, CHUNK, size), f32),
            pltpu.VMEM((capacity, size), f32),
            pltpu.VMEM((size, size), f32),
            pltpu.VMEM((n_texel, first, size), f32), pltpu.VMEM((n_texel, rest, size), f32),
            pltpu.VMEM((n_texel, first, size), f32), pltpu.VMEM((n_texel, rest, size), f32),
            pltpu.VMEM((2, first, size), f32), pltpu.VMEM((2, rest, size), f32),
            pltpu.VMEM((n_texel, first, size), f32), pltpu.VMEM((n_texel, rest, size), f32),
            sems((2, chunks)), sems((2, chunks)),
            sems((2, direct)), sems((2, n_light, direct)),
            sems((2, chunks)), sems((2, chunks)),
            sems((2, n_texel)), sems((2, n_texel)),
            sems((2, n_light)), sems((2, 2)),
            sems((2, n_texel)), sems((2, n_texel)),
            sems((2, bits, n_texel)), sems((2, bits, n_texel)),
        ],
        compiler_params=pltpu.CompilerParams(collective_id=1, has_side_effects=True),
    )(tex_feat, light_feat, sketch, row_counts)
    return pl.pallas_call(
        write_out,
        out_shape=(jax.ShapeDtypeStruct((capacity, size), f32), jax.ShapeDtypeStruct((piece, lights), f32)),
        in_specs=[vmem, vmem],
        out_specs=(pl.BlockSpec(memory_space=pl.ANY),) * 2,
        scratch_shapes=[sems((2,))],
    )(*(pltpu.with_memory_space_constraint(x, pltpu.VMEM) for x in (basis, coeffs)))


def solution(mesh):
    placed = (P("texel", None), P("light", None), P("light", None), P())
    return jax.shard_map(
        functools.partial(on_device, mesh.shape["texel"], mesh.shape["light"]),
        mesh=mesh,
        in_specs=placed,
        out_specs=(P("texel", None), P("texel", "light")),
        check_vma=False,
    )
```

```python
import functools

import jax
import jax.numpy as jnp
from jax import lax
from jax.experimental import pallas as pl
from jax.experimental.pallas import tpu as pltpu
from jax.sharding import PartitionSpec as P

HIGHEST = lax.Precision.HIGHEST
BLOCK = 64
CHUNK = 16
INV_TWO_PI = 0.15915494309189535
SINE = (6.283185273788226, -41.34167747777608, 81.60223120329199, -76.57499125549666, 39.71091094809089)


def bounded_sine(x):
    turns = x * INV_TWO_PI - 0.25
    z = 0.25 - jnp.abs(turns - jnp.round(turns))
    s = z * z
    value = SINE[-1] * s + SINE[-2]
    for coefficient in SINE[-3::-1]:
        value = value * s + coefficient
    return value * z


def eliminate(block):
    rows = [block[8 * t : 8 * t + 8, :] for t in range(8)]
    below = lax.broadcasted_iota(jnp.int32, (8, 128), 0)

    def line_of(value, k):
        return jnp.broadcast_to(value[k : k + 1, :], (8, 128))

    def lane_of(value, k):
        return jnp.broadcast_to(value[:, k : k + 1], (8, 128))

    own = [lane_of(rows[0], k) for k in range(8)]
    for p in range(8):
        columns = {(t, k): lane_of(rows[t], 8 * p + k) for t in range(p + 1, 8) for k in range(8)}
        ahead = [lane_of(rows[p + 1], 8 * p + 8 + k) for k in range(8)] if p < 7 else None
        for k in range(8):
            inverse = 1.0 / line_of(own[k], k)
            factor = jnp.where(below > k, own[k] * inverse, 0.0)
            entries = {later: line_of(own[later], k) for later in range(k + 1, 8)}
            for later, entry in entries.items():
                own[later] = own[later] - factor * entry
            pivot_row = line_of(rows[p], k)
            rows[p] = rows[p] - factor * pivot_row
            for t in range(p + 1, 8):
                factor = columns[t, k] * inverse
                if t == p + 1:
                    for later in range(8):
                        ahead[later] = ahead[later] - factor * line_of(columns[t, k], later)
                for later, entry in entries.items():
                    columns[t, later] = columns[t, later] - factor * entry
                rows[t] = rows[t] - factor * pivot_row
        own = ahead
    return jnp.concatenate(rows, axis=0)


def factor_inverse(work_ref, finish_gram):
    size = work_ref.shape[0]
    row = lax.broadcasted_iota(jnp.int32, (size, size), 0)
    column = lax.broadcasted_iota(jnp.int32, (size, size), 1)
    work_ref[:, size:] = jnp.where(row == column, 1.0, 0.0).astype(jnp.float32)
    lane = lax.broadcasted_iota(jnp.int32, (BLOCK, 128), 1)
    line = lax.broadcasted_iota(jnp.int32, (BLOCK, 128), 0)
    for start in range(0, size, BLOCK):
        own = slice(start, start + BLOCK)
        first = start // 128 * 128
        last = size + (start + BLOCK + 127) // 128 * 128
        tile = work_ref[own, first : first + 128]
        if start % 128:
            tile = pltpu.roll(tile, 64, 1)
        unit = jnp.where(lane - BLOCK == line, 1.0, 0.0)
        done = eliminate(jnp.where(lane < BLOCK, tile, unit))
        pivots = jnp.sum(jnp.where(lane == line, done, 0.0), axis=1, keepdims=True)
        scaled = pltpu.roll(done * lax.rsqrt(pivots), 64, 1)[:, :BLOCK]
        both = jnp.dot(scaled, work_ref[own, first:last], precision=HIGHEST, preferred_element_type=jnp.float32)
        work_ref[own, size:last] = both[:, size - first :]
        if start == 0:
            finish_gram()
        flipped = both[:, : size - first].T
        for lower in ((start + BLOCK, start + 2 * BLOCK), (start + 2 * BLOCK, size)):
            if lower[0] < min(lower[1], size):
                work_ref[lower[0] : lower[1], first:last] -= jnp.dot(
                    flipped[lower[0] - first : lower[1] - first, :], both,
                    precision=HIGHEST, preferred_element_type=jnp.float32,
                )


def split(value):
    high = value.astype(jnp.bfloat16)
    return high, (value - high.astype(jnp.float32)).astype(jnp.bfloat16)


def product(left, right):
    def one(a, b):
        return lax.dot_general(a, b, (((1,), (1,)), ((), ())), preferred_element_type=jnp.float32)

    return one(left[0], right[0]) + (one(left[0], right[1]) + one(left[1], right[0]))


MESH_ID = pl.DeviceIdType.MESH


def relay_order(chunks):
    hop = 0.29 * chunks
    events = [(c, "inward", c) for c in range(chunks)]
    events += [(c + hop, "outward", c) for c in range(chunks)]
    events += [(c + max(3 * hop, chunks + 3), "back_inward", c) for c in range(chunks)]
    events += [(c + hop + chunks + 1, "back_outward", c) for c in range(chunks)]
    events += [(hop + 1.7 * chunks + 4 * g, "column", g) for g in range(2)]
    return [(kind, c) for _, kind, c in sorted(events)]


def whole_step(
    n_texel, n_light, tex_hbm, feat_hbm, sketch_hbm, counts_hbm, basis_hbm, coeffs_hbm,
    tex_ref, feat_ref, sketch_ref, counts_ref, basis_ref, coeffs_ref,
    tile_ref, half_ref, product_ref, held, arrived,
    logits_even, logits_odd, partial_ref,
    landed, whole, work, gram, high, low,
    pieces_first, pieces_rest, plane_first, plane_rest, column_first, column_rest, rows_first, rows_rest,
    sum_send, back_send, chunk_recv,
    plane_send, plane_recv, column_send, column_recv, row_send, row_recv, out_send, out_recv,
    local_sems, tex_sems,
):
    texel, light = lax.axis_index("texel"), lax.axis_index("light")
    capacity, size = partial_ref.shape
    width = logits_even.shape[1]
    block = logits_even.shape[0]
    middle = capacity // 2
    chunks = middle // CHUNK
    upper = light // (n_light // 2)
    inward, outward = 1 - upper, upper
    blocks = middle // block
    turns = [(inward, 0, block // 2), (inward, block // 2, block // 2)]
    turns += [(inward, b * block, block) for b in range(1, blocks)]
    turns += [(outward, b * block, block) for b in range(blocks)]

    def turn_rows(half, offset, height):
        return pl.ds(pl.multiple_of(half * middle + offset, height), height)

    tex_copies = [
        pltpu.make_async_copy(tex_hbm.at[turn_rows(*turn)], tex_ref.at[turn_rows(*turn)], tex_sems.at[index])
        for index, turn in enumerate(turns)
    ]
    feat_copies = [
        pltpu.make_async_copy(
            feat_hbm.at[pl.ds(c * width, width)], feat_ref.at[pl.ds(c * width, width)], local_sems.at[4]
        )
        for c in range(feat_ref.shape[0] // width)
    ]
    sketch_copy = pltpu.make_async_copy(sketch_hbm, sketch_ref, local_sems.at[2])
    counts_copy = pltpu.make_async_copy(counts_hbm, counts_ref, local_sems.at[3])
    for going in tex_copies[:1] + feat_copies + [counts_copy, sketch_copy]:
        going.start()
    lights = [lax.rem(light + d, n_light) for d in range(n_light)]
    texels = [lax.rem(texel + d, n_texel) for d in range(n_texel)]
    depth = light + upper * (n_light - 1 - 2 * light)
    inner = 1 - (n_light // 2 - depth) // (n_light // 2)
    toward_middle = light + 1 - 2 * upper
    toward_end = light - 1 + 2 * upper

    barrier = pltpu.get_barrier_semaphore()
    peers = [(texel, lights[d]) for d in range(1, n_light)] + [(texels[d], light) for d in range(1, n_texel)]
    for peer in peers:
        pl.semaphore_signal(barrier, inc=1, device_id=peer, device_id_type=MESH_ID)

    def copy(source, target, send_sem, recv_sem, device):
        return pltpu.make_async_remote_copy(
            src_ref=source, dst_ref=target, send_sem=send_sem, recv_sem=recv_sem,
            device_id=device, device_id_type=MESH_ID,
        )

    def chunk_rows(half, c):
        return pl.ds(pl.multiple_of(half * middle + c * CHUNK, CHUNK), CHUNK)

    def sum_copy(half, c, to):
        return copy(
            partial_ref.at[chunk_rows(half, c)], landed.at[half, c],
            sum_send.at[half], chunk_recv.at[half, c], (texel, to),
        )

    def all_sent(ref, sems, half):
        rows = ref.at[pl.ds(pl.multiple_of(half * middle, middle), middle)]
        copy(rows, rows, sems.at[half], chunk_recv.at[half, 0], (texel, toward_middle)).wait_send()

    def back_copy(half, c, to):
        rows = chunk_rows(half, c)
        return copy(
            whole.at[rows], whole.at[rows], back_send.at[half], chunk_recv.at[half, c], (texel, to)
        )

    def fill(turn):
        half, offset, height = turns[turn]
        rows = turn_rows(half, offset, height)
        logits = (logits_even.at[pl.ds(0, height)], logits_odd.at[pl.ds(0, height)])
        count = feat_ref.shape[0] // width

        def product_of(c):
            return lax.dot_general(
                tex_ref[rows, :], feat_ref[c * width : (c + 1) * width, :], (((1,), (1,)), ((), ())),
                preferred_element_type=jnp.float32,
            )

        tex_copies[turn].wait()
        if turn == 0:
            pltpu.make_async_copy(feat_hbm, feat_ref, local_sems.at[4]).wait()
            for going in tex_copies[1:]:
                going.start()
        logits[0][...] = product_of(0)
        for c in range(count):
            if c + 1 < count:
                logits[(c + 1) % 2][...] = product_of(c + 1)
            tile_ref[rows, c * width : (c + 1) * width] = bounded_sine(logits[c % 2][...]).astype(jnp.bfloat16)
        if turn == 0:
            sketch_copy.wait()
            counts_copy.wait()
        own_count = counts_ref[texel]
        slot = half * middle + offset + lax.broadcasted_iota(jnp.int32, (height, size), 0)
        sums = jnp.dot(tile_ref[rows, :], sketch_ref[...], preferred_element_type=jnp.float32)
        partial_ref[rows, :] = jnp.where(slot < own_count, sums, 0.0)

    for turn, (_, offset, height) in enumerate(turns):
        fill(turn)
        if turn == 0:
            pl.semaphore_wait(barrier, len(peers))

        @pl.when(inner == 0)
        def _():
            if turn <= blocks:
                for c in range(offset // CHUNK, (offset + height) // CHUNK):
                    sum_copy(inward, c, toward_middle).start()

    def split_half(half):
        for index in range(blocks):
            rows = turn_rows(half, index * block, block)
            high[rows, :], low[rows, :] = split(whole[rows, :])

    groups = (
        (pieces_first, plane_first, column_first, rows_first),
        (pieces_rest, plane_rest, column_rest, rows_rest),
    )
    quarter = size // 4

    def column_wait(g, side):
        column = groups[g][2]
        copy(
            column.at[side], column.at[side], column_send.at[g], column_recv.at[g, side], (texel, lights[1])
        ).wait_recv()

    def spread_rows(g):
        _, _, column, rows = groups[g]
        column_wait(g, 1 - upper)
        rows[texel] = column[0] + column[1]
        for d in range(1, n_texel):
            copy(rows.at[texel], rows.at[texel], row_send.at[g], row_recv.at[g], (texels[d], light)).start()

    @pl.when(inner == 0)
    def _():
        done = 0
        for c in range(chunks):
            rows = chunk_rows(outward, c)
            sum_copy(outward, c, toward_middle).wait_recv()
            whole[rows, :] = partial_ref[rows, :] + landed[outward, c]
            if c == 0:
                all_sent(partial_ref, sum_send, inward)
            back_copy(outward, c, toward_middle).start()
            if c + 1 in (chunks // 2, chunks * 3 // 4, chunks):
                height = (c + 1 - done) * CHUNK
                own = whole[pl.ds(pl.multiple_of(outward * middle + done * CHUNK, CHUNK), height), :]
                some = lax.dot_general(
                    own, own, (((0,), (0,)), ((), ())), precision=HIGHEST, preferred_element_type=jnp.float32
                )
                gram[...] = some if done == 0 else gram[...] + some
                done = c + 1
        local = gram[...]
        rest = jnp.concatenate(
            [local[2 * quarter : 3 * quarter, 2 * quarter :], local[3 * quarter :, 2 * quarter :]], axis=1
        )
        rest = jnp.concatenate([local[quarter : 2 * quarter, :], rest], axis=0)
        for index in range(n_texel):
            for part, ref in ((local, pieces_first), (rest, pieces_rest)):
                height = ref.shape[1]
                ref[index] = part[index * height : (index + 1) * height, :]
        copies = [
            [
                copy(
                    pieces.at[texels[d]], plane.at[d], plane_send.at[g], plane_recv.at[g], (texels[d], light)
                )
                for d in range(1, n_texel)
            ]
            for g, (pieces, plane, _, _) in enumerate(groups)
        ]
        for going in copies[0] + copies[1]:
            going.start()
        split_half(outward)
        for g, (pieces, plane, column, _) in enumerate(groups):
            total = pieces[texel]
            others = pl.ds(1, n_texel - 1)
            copy(pieces.at[others], plane.at[others], plane_send.at[g], plane_recv.at[g], (texels[1], light)).wait()
            for d in range(1, n_texel):
                total = total + plane[d]
            column[upper] = total
            for d in range(1, n_light):
                copy(
                    column.at[upper], column.at[upper], column_send.at[g], column_recv.at[g, upper],
                    (texel, lights[d]),
                ).start()
        for g in range(2):
            spread_rows(g)

    @pl.when(inner == 1)
    def _():
        for kind, c in relay_order(chunks):
            if kind == "column":
                column_wait(c, upper)
                spread_rows(c)
            elif kind == "inward" or kind == "outward":
                half, to = (inward, toward_middle) if kind == "inward" else (outward, toward_end)
                going = sum_copy(half, c, to)
                going.wait_recv()
                rows = chunk_rows(half, c)
                partial_ref[rows, :] = partial_ref[rows, :] + landed[half, c]
                going.start()
            else:
                half, to = (outward, toward_middle) if kind == "back_inward" else (inward, toward_end)
                going = back_copy(half, c, to)
                going.wait_recv()
                going.start()
        split_half(inward)
        split_half(outward)

    def row_whole(g):
        others = groups[g][3].at[pl.ds(1, n_texel - 1)]
        return copy(others, others, row_send.at[g], row_recv.at[g], (texels[1], light))

    valid = counts_ref[0]
    for index in range(1, n_texel):
        valid = valid + counts_ref[index]
    valid = valid.astype(jnp.float32)
    row_whole(0).wait_recv()
    height = rows_first.shape[1]
    for index in range(n_texel):
        work[index * height : (index + 1) * height, :size] = rows_first[index] / valid

    def finish_gram():
        @pl.when(inner == 0)
        def _():
            for c in range(chunks):
                back_copy(inward, c, toward_middle).wait_recv()

            split_half(inward)

        row_whole(1).wait_recv()
        height = rows_rest.shape[1]
        rest = jnp.concatenate([rows_rest[index] for index in range(n_texel)], axis=0) / valid
        work[quarter : 2 * quarter, :size] = rest[:quarter, :]
        work[2 * quarter :, : 2 * quarter] = jnp.zeros((2 * quarter, 2 * quarter), jnp.float32)
        work[2 * quarter : 3 * quarter, 2 * quarter : size] = rest[quarter:, : 2 * quarter]
        work[3 * quarter :, 2 * quarter : size] = rest[quarter:, 2 * quarter :]

    factor_inverse(work, finish_gram)
    inverse = split(work[:, size:])
    half_ref[...] = product(inverse, (high[...], low[...])).astype(jnp.bfloat16)
    basis_out = pltpu.make_async_copy(basis_ref, basis_hbm, local_sems.at[0])

    def basis_rows(step):
        rows = slice(step * middle, (step + 1) * middle)
        basis_ref[rows, :] = product((high[rows, :], low[rows, :]), inverse)
        if step == 1:
            basis_out.start()

    scatter_sum(
        n_texel, half_ref, tile_ref, product_ref, coeffs_ref, valid, held, arrived, out_send, out_recv, basis_rows
    )
    coeffs_out = pltpu.make_async_copy(coeffs_ref, coeffs_hbm, local_sems.at[1])
    coeffs_out.start()
    for half in range(2):
        sent = held.at[half, pl.ds(0, n_texel - 1)]
        copy(sent, sent, out_send.at[half], out_recv.at[half, 0], (texels[1], light)).wait_send()

    @pl.when(inner == 0)
    def _():
        all_sent(whole, back_send, outward)
        for g in range(2):
            sent = groups[g][1].at[pl.ds(0, n_light - 1)]
            copy(sent, sent, column_send.at[g], column_recv.at[g, upper], (texel, lights[1])).wait_send()

    @pl.when(inner == 1)
    def _():
        for half in (inward, outward):
            all_sent(partial_ref, sum_send, half)
            all_sent(whole, back_send, half)

    for g in range(2):
        row_whole(g).wait_send()
    basis_out.wait()
    coeffs_out.wait()


def halving_order(bits, last_first):
    rest = list(range(1, bits))
    return [0] + (rest[::-1] if last_first else rest)


def scatter_sum(n_texel, half_ref, tile_ref, partial_ref, out_ref, valid, held, landed, send_sem, recv_sem, meanwhile):
    texel, light = lax.axis_index("texel"), lax.axis_index("light")
    bits = n_texel.bit_length() - 1
    bit = [lax.rem(texel // (1 << b), 2) for b in range(bits)]
    partner = [texel + (1 - 2 * bit[b]) * (1 << b) for b in range(bits)]
    piece = partial_ref.shape[0] // n_texel
    width = partial_ref.shape[1] // 2

    def start_of(mask):
        block = 0
        for b in range(bits):
            flipped = 1 - bit[b] if mask >> b & 1 else bit[b]
            block = block + flipped * (1 << b)
        return pl.multiple_of(block * piece, piece)

    def multiply(half):
        columns = slice(half * width, (half + 1) * width)
        partial_ref[:, columns] = lax.dot_general(
            half_ref[...], tile_ref[:, columns], (((1,), (0,)), ((), ())), preferred_element_type=jnp.float32
        )

    orders = [halving_order(bits, False), halving_order(bits, True)]
    root = jnp.sqrt(jnp.full((piece, width), valid))
    flights = [{}, {}]
    used = [0, 0]
    for step in range(bits):
        for half, order in enumerate(orders):
            if step == 0:
                multiply(half)
            b = order[step]
            left = [m for m in range(n_texel) if all(not m >> done & 1 for done in order[:step])]
            later = order[step + 1 :]
            going = [m for m in left if m >> b & 1]
            going.sort(key=lambda m: [-(m >> c & 1) for c in later])
            columns = pl.ds(half * width, width)
            for m in going:
                kept = m - (1 << b)
                if step == 0:
                    source = partial_ref.at[pl.ds(start_of(m), piece), columns]
                else:
                    arrived = flights[half].pop((step - 1, m))
                    arrived.wait_recv()
                    below = (
                        partial_ref[pl.ds(start_of(m), piece), columns] if step == 1 else held[half, m]
                    )
                    held[half, m] = below + landed[half, step - 1, m]
                    source = held.at[half, m]
                copy = pltpu.make_async_remote_copy(
                    src_ref=source,
                    dst_ref=landed.at[half, step, kept],
                    send_sem=send_sem.at[half],
                    recv_sem=recv_sem.at[half, used[half]],
                    device_id=(partner[b], light),
                    device_id_type=MESH_ID,
                )
                copy.start()
                used[half] += 1
                flights[half][step, kept] = copy
        if step < 2:
            meanwhile(step)
        if step:
            for half, order in enumerate(orders):
                for key in [k for k in flights[half] if k[0] == step - 1]:
                    m = key[1]
                    flights[half].pop(key).wait_recv()
                    columns = pl.ds(half * width, width)
                    below = (
                        partial_ref[pl.ds(start_of(m), piece), columns] if step == 1 else held[half, m]
                    )
                    held[half, m] = below + landed[half, step - 1, m]
    for half in range(2):
        columns = pl.ds(half * width, width)
        flights[half].pop((bits - 1, 0)).wait_recv()
        below = partial_ref[pl.ds(start_of(0), piece), columns] if bits == 1 else held[half, 0]
        out_ref[:, half * width : (half + 1) * width] = (below + landed[half, bits - 1, 0]) / root


def write_out(basis_ref, coeffs_ref, basis_out, coeffs_out, sems):
    copies = [
        pltpu.make_async_copy(basis_ref, basis_out, sems.at[0]),
        pltpu.make_async_copy(coeffs_ref, coeffs_out, sems.at[1]),
    ]
    for going in copies:
        going.start()
    for going in copies:
        going.wait()


def on_device(n_texel, n_light, tex_feat, light_feat, sketch, row_counts):
    capacity, size = tex_feat.shape[0], sketch.shape[1]
    lights = light_feat.shape[0]
    block, step = capacity // 4, next(w for w in (256, 128) if lights % w == 0)
    chunks, piece = capacity // 2 // CHUNK, size // n_texel
    first, rest = size // 4 // n_texel, size // 2 // n_texel
    width, bits = lights // 2, n_texel.bit_length() - 1
    vmem = pl.BlockSpec(memory_space=pltpu.VMEM)
    anywhere = pl.BlockSpec(memory_space=pl.ANY)
    f32, half = jnp.float32, jnp.bfloat16
    sems = pltpu.SemaphoreType.DMA
    basis, coeffs = pl.pallas_call(
        functools.partial(whole_step, n_texel, n_light),
        out_shape=(pltpu.VMEM((capacity, size), f32), pltpu.VMEM((piece, lights), f32)),
        in_specs=[anywhere] * 4,
        out_specs=(anywhere, anywhere),
        scratch_shapes=[
            pltpu.VMEM(tex_feat.shape, half),
            pltpu.VMEM(light_feat.shape, half),
            pltpu.VMEM(sketch.shape, half),
            pltpu.SMEM(row_counts.shape, jnp.int32),
            pltpu.VMEM((capacity, size), f32),
            pltpu.VMEM((piece, lights), f32),
            pltpu.VMEM((capacity, lights), half),
            pltpu.VMEM((size, capacity), half),
            pltpu.VMEM((size, lights), f32),
            pltpu.VMEM((2, n_texel, piece, width), f32),
            pltpu.VMEM((2, bits, n_texel, piece, width), f32),
            pltpu.VMEM((block, step), f32),
            pltpu.VMEM((block, step), f32),
            pltpu.VMEM((capacity, size), f32),
            pltpu.VMEM((2, chunks, CHUNK, size), f32),
            pltpu.VMEM((capacity, size), f32),
            pltpu.VMEM((size, 2 * size), f32),
            pltpu.VMEM((size, size), f32),
            pltpu.VMEM((capacity, size), half),
            pltpu.VMEM((capacity, size), half),
            pltpu.VMEM((n_texel, first, size), f32), pltpu.VMEM((n_texel, rest, size), f32),
            pltpu.VMEM((n_texel, first, size), f32), pltpu.VMEM((n_texel, rest, size), f32),
            pltpu.VMEM((2, first, size), f32), pltpu.VMEM((2, rest, size), f32),
            pltpu.VMEM((n_texel, first, size), f32), pltpu.VMEM((n_texel, rest, size), f32),
            sems((2,)), sems((2,)), sems((2, chunks)),
            sems((2,)), sems((2,)),
            sems((2,)), sems((2, 2)),
            sems((2,)), sems((2,)),
            sems((2,)), sems((2, n_texel - 1)),
            sems((5,)), sems((5,)),
        ],
        compiler_params=pltpu.CompilerParams(collective_id=1, has_side_effects=True),
    )(tex_feat, light_feat, sketch, row_counts)
    return pl.pallas_call(
        write_out,
        out_shape=(jax.ShapeDtypeStruct((capacity, size), f32), jax.ShapeDtypeStruct((piece, lights), f32)),
        in_specs=[vmem, vmem],
        out_specs=(pl.BlockSpec(memory_space=pl.ANY),) * 2,
        scratch_shapes=[sems((2,))],
    )(*(pltpu.with_memory_space_constraint(x, pltpu.VMEM) for x in (basis, coeffs)))


def solution(mesh):
    placed = (P("texel", None), P("light", None), P("light", None), P())
    return jax.shard_map(
        functools.partial(on_device, mesh.shape["texel"], mesh.shape["light"]),
        mesh=mesh,
        in_specs=placed,
        out_specs=(P("texel", None), P("texel", "light")),
        check_vma=False,
    )
```

```python
import functools

import jax
import jax.numpy as jnp
from jax import lax
from jax.experimental import pallas as pl
from jax.experimental.pallas import tpu as pltpu
from jax.sharding import PartitionSpec as P

HIGHEST = lax.Precision.HIGHEST
BLOCK = 64
CHUNK = 16
INV_TWO_PI = 0.15915494309189535
SINE = (6.283185273788226, -41.34167747777608, 81.60223120329199, -76.57499125549666, 39.71091094809089)


def bounded_sine(x):
    turns = x * INV_TWO_PI - 0.25
    z = 0.25 - jnp.abs(turns - jnp.round(turns))
    s = z * z
    value = SINE[-1] * s + SINE[-2]
    for coefficient in SINE[-3::-1]:
        value = value * s + coefficient
    return value * z


def eliminate(block):
    rows = [block[8 * t : 8 * t + 8, :] for t in range(8)]
    below = lax.broadcasted_iota(jnp.int32, (8, 128), 0)

    def line_of(value, k):
        return jnp.broadcast_to(value[k : k + 1, :], (8, 128))

    def lane_of(value, k):
        return jnp.broadcast_to(value[:, k : k + 1], (8, 128))

    own = [lane_of(rows[0], k) for k in range(8)]
    for p in range(8):
        columns = {(t, k): lane_of(rows[t], 8 * p + k) for t in range(p + 1, 8) for k in range(8)}
        ahead = [lane_of(rows[p + 1], 8 * p + 8 + k) for k in range(8)] if p < 7 else None
        for k in range(8):
            inverse = 1.0 / line_of(own[k], k)
            factor = jnp.where(below > k, own[k] * inverse, 0.0)
            entries = {later: line_of(own[later], k) for later in range(k + 1, 8)}
            for later, entry in entries.items():
                own[later] = own[later] - factor * entry
            pivot_row = line_of(rows[p], k)
            rows[p] = rows[p] - factor * pivot_row
            for t in range(p + 1, 8):
                factor = columns[t, k] * inverse
                if t == p + 1:
                    for later in range(8):
                        ahead[later] = ahead[later] - factor * line_of(columns[t, k], later)
                for later, entry in entries.items():
                    columns[t, later] = columns[t, later] - factor * entry
                rows[t] = rows[t] - factor * pivot_row
        own = ahead
    return jnp.concatenate(rows, axis=0)


def factor_inverse(work_ref, finish_gram, finish_rows):
    size = work_ref.shape[0]
    row = lax.broadcasted_iota(jnp.int32, (size, size), 0)
    column = lax.broadcasted_iota(jnp.int32, (size, size), 1)
    work_ref[:, size:] = jnp.where(row == column, 1.0, 0.0).astype(jnp.float32)
    lane = lax.broadcasted_iota(jnp.int32, (BLOCK, 128), 1)
    line = lax.broadcasted_iota(jnp.int32, (BLOCK, 128), 0)
    for start in range(0, size, BLOCK):
        own = slice(start, start + BLOCK)
        first = start // 128 * 128
        last = size + (start + BLOCK + 127) // 128 * 128
        tile = work_ref[own, first : first + 128]
        if start % 128:
            tile = pltpu.roll(tile, 64, 1)
        unit = jnp.where(lane - BLOCK == line, 1.0, 0.0)
        done = eliminate(jnp.where(lane < BLOCK, tile, unit))
        pivots = jnp.sum(jnp.where(lane == line, done, 0.0), axis=1, keepdims=True)
        scaled = pltpu.roll(done * lax.rsqrt(pivots), 64, 1)[:, :BLOCK]
        both = jnp.dot(scaled, work_ref[own, first:last], precision=HIGHEST, preferred_element_type=jnp.float32)
        work_ref[own, size:last] = both[:, size - first :]
        if start == 0:
            finish_gram()
        if start == 2 * BLOCK:
            finish_rows()
        flipped = both[:, : size - first].T
        for lower in ((start + BLOCK, start + 2 * BLOCK), (start + 2 * BLOCK, size)):
            if lower[0] < min(lower[1], size):
                work_ref[lower[0] : lower[1], first:last] -= jnp.dot(
                    flipped[lower[0] - first : lower[1] - first, :], both,
                    precision=HIGHEST, preferred_element_type=jnp.float32,
                )


def split(value):
    high = value.astype(jnp.bfloat16)
    return high, (value - high.astype(jnp.float32)).astype(jnp.bfloat16)


def product(left, right):
    def one(a, b):
        return lax.dot_general(a, b, (((1,), (1,)), ((), ())), preferred_element_type=jnp.float32)

    return one(left[0], right[0]) + (one(left[0], right[1]) + one(left[1], right[0]))


MESH_ID = pl.DeviceIdType.MESH


def layout_of(capacity, n_light):
    count = capacity // CHUNK
    if n_light == 4:
        shares = [count * 3 // 8, count // 8, count // 8, count * 3 // 8]
    else:
        shares = [count // 2] + [0] * (n_light - 2) + [count // 2]
    return shares, [sum(shares[:z]) for z in range(n_light)]


def relay_order(shares):
    far, ends, owned = len(shares) - 1, shares[0], shares[1]
    outgoing = [(far, c) for c in range(ends)] + [(2, c) for c in range(owned)]
    hop = 8.3 if owned else 0.29 * ends
    last = ends + owned + 2 * hop
    events = [(i + hop, "inward", o, c) for i, (o, c) in enumerate(outgoing)]
    events += [(c + 2 * hop, "outward", 0, c) for c in range(ends)]
    if owned:
        events += [(ends + c + 2 * hop, "final", 1, c) for c in range(owned)]
        events += [(ends + c + 3 * hop, "back_outward", 2, c) for c in range(owned)]
        events += [(last + 0.5, "plane", 0, 0), (last + 12.5, "column", 0, 0)]
    events += [(last + 2 + c, "back_inward", 0, c) for c in range(ends)]
    events += [(last + 2 + hop + c, "back_outward", far, c) for c in range(ends)]
    events += [(last + 22 + 3 * g, "rows", 0, g) for g in range(2)]
    return [event[1:] for event in sorted(events)]


def whole_step(
    n_texel, n_light, tex_hbm, feat_hbm, sketch_hbm, counts_hbm, basis_hbm, coeffs_hbm,
    tex_ref, feat_ref, sketch_ref, counts_ref, basis_ref, coeffs_ref,
    tile_ref, half_ref, product_ref, held, arrived,
    logits_even, logits_odd, partial_ref,
    landed, near, whole, work, gram, high, low,
    pieces_first, pieces_rest, plane_first, plane_rest, column_first, column_rest, rows_first, rows_rest,
    sum_send, back_send, chunk_recv, near_recv,
    plane_send, plane_recv, column_send, column_recv, row_send, row_recv, out_send, out_recv,
    local_sems, tex_sems,
):
    texel, light = lax.axis_index("texel"), lax.axis_index("light")
    capacity, size = partial_ref.shape
    width = logits_even.shape[1]
    block = logits_even.shape[0]
    middle = capacity // 2
    shares, starts = layout_of(capacity, n_light)
    far, ends, owned = n_light - 1, shares[0], shares[1]
    owners = column_first.shape[0]
    upper = light // (n_light // 2)

    def chunk_of(o, c):
        return starts[o] + c + upper * (starts[far - o] - starts[o])

    def rows_at(o, c, height):
        return pl.ds(pl.multiple_of(chunk_of(o, c) * CHUNK, CHUNK), height)

    half_block = block // 2
    per_half = half_block // CHUNK
    turns = [(rows_at(far, 0, half_block), half_block, [(far, c) for c in range(per_half)])]
    if owned:
        turns += [(rows_at(far, per_half, block), block, [(far, c) for c in range(per_half, ends)])]
        shared = pl.ds(starts[1] * CHUNK, block)
        turns += [(shared, block, [(o, c) for o in (2, 1) for c in range(owned)])]
        turns += [(rows_at(0, 0, block), block, []), (rows_at(0, 2 * per_half, half_block), half_block, [])]
    else:
        turns += [(rows_at(far, per_half, half_block), half_block, [(far, per_half + c) for c in range(per_half)])]
        turns += [(rows_at(far, 2 * per_half, block), block, [(far, c) for c in range(2 * per_half, ends)])]
        turns += [(rows_at(0, 0, block), block, []), (rows_at(0, 2 * per_half, block), block, [])]

    tex_copies = [
        pltpu.make_async_copy(tex_hbm.at[rows], tex_ref.at[rows], tex_sems.at[index])
        for index, (rows, _, _) in enumerate(turns)
    ]
    feat_copies = [
        pltpu.make_async_copy(
            feat_hbm.at[pl.ds(c * width, width)], feat_ref.at[pl.ds(c * width, width)], local_sems.at[4]
        )
        for c in range(feat_ref.shape[0] // width)
    ]
    sketch_copy = pltpu.make_async_copy(sketch_hbm, sketch_ref, local_sems.at[2])
    counts_copy = pltpu.make_async_copy(counts_hbm, counts_ref, local_sems.at[3])
    for going in tex_copies[:1] + feat_copies + [counts_copy, sketch_copy]:
        going.start()
    lights = [lax.rem(light + d, n_light) for d in range(n_light)]
    texels = [lax.rem(texel + d, n_texel) for d in range(n_texel)]
    depth = light + upper * (n_light - 1 - 2 * light)
    inner = 1 - (n_light // 2 - depth) // (n_light // 2)
    inward, outward = light + 1 - 2 * upper, light - 1 + 2 * upper

    barrier = pltpu.get_barrier_semaphore()
    peers = [(texel, lights[d]) for d in range(1, n_light)] + [(texels[d], light) for d in range(1, n_texel)]
    for peer in peers:
        pl.semaphore_signal(barrier, inc=1, device_id=peer, device_id_type=MESH_ID)

    def copy(source, target, send_sem, recv_sem, device):
        return pltpu.make_async_remote_copy(
            src_ref=source, dst_ref=target, send_sem=send_sem, recv_sem=recv_sem,
            device_id=device, device_id_type=MESH_ID,
        )

    def sum_copy(o, c, to):
        chunk = chunk_of(o, c)
        return copy(
            partial_ref.at[rows_at(o, c, CHUNK)], landed.at[chunk], sum_send, chunk_recv.at[chunk], (texel, to)
        )

    def near_copy(c, to):
        return copy(partial_ref.at[rows_at(1, c, CHUNK)], near.at[c], sum_send, near_recv.at[c], (texel, to))

    def back_copy(o, c, to):
        rows = rows_at(o, c, CHUNK)
        return copy(whole.at[rows], whole.at[rows], back_send, chunk_recv.at[chunk_of(o, c)], (texel, to))

    def all_sent(sem, chunks):
        while chunks:
            some = min(chunks, capacity // CHUNK)
            sent = whole.at[pl.ds(0, some * CHUNK)]
            copy(sent, sent, sem, chunk_recv.at[0], (texel, inward)).wait_send()
            chunks -= some

    def fill(turn):
        rows, height, _ = turns[turn]
        logits = (logits_even.at[pl.ds(0, height)], logits_odd.at[pl.ds(0, height)])
        count = feat_ref.shape[0] // width

        def product_of(c):
            return lax.dot_general(
                tex_ref[rows, :], feat_ref[c * width : (c + 1) * width, :], (((1,), (1,)), ((), ())),
                preferred_element_type=jnp.float32,
            )

        tex_copies[turn].wait()
        if turn == 0:
            pltpu.make_async_copy(feat_hbm, feat_ref, local_sems.at[4]).wait()
            for going in tex_copies[1:]:
                going.start()
        logits[0][...] = product_of(0)
        for c in range(count):
            if c + 1 < count:
                logits[(c + 1) % 2][...] = product_of(c + 1)
            tile_ref[rows, c * width : (c + 1) * width] = bounded_sine(logits[c % 2][...]).astype(jnp.bfloat16)
        if turn == 0:
            sketch_copy.wait()
            counts_copy.wait()
        own_count = counts_ref[texel]
        slot = rows.start + lax.broadcasted_iota(jnp.int32, (height, size), 0)
        sums = jnp.dot(tile_ref[rows, :], sketch_ref[...], preferred_element_type=jnp.float32)
        partial_ref[rows, :] = jnp.where(slot < own_count, sums, 0.0)

    for turn, (_, _, ready) in enumerate(turns):
        fill(turn)
        if turn == 0:
            pl.semaphore_wait(barrier, len(peers))

        @pl.when(inner == 0)
        def _():
            for o, c in ready:
                (near_copy(c, inward) if o == 1 and owned else sum_copy(o, c, inward)).start()

    def split_rows(o):
        if shares[o]:
            rows = rows_at(o, 0, shares[o] * CHUNK)
            high[rows, :], low[rows, :] = split(whole[rows, :])

    groups = (
        (pieces_first, plane_first, column_first, rows_first),
        (pieces_rest, plane_rest, column_rest, rows_rest),
    )
    quarter = size // 4
    own_column = light if owned else upper

    def add_gram(o, first, chunks):
        own = whole[rows_at(o, first, chunks * CHUNK), :]
        some = lax.dot_general(
            own, own, (((0,), (0,)), ((), ())), precision=HIGHEST, preferred_element_type=jnp.float32
        )
        gram[...] = gram[...] + some if first else some

    def plane_start():
        local = gram[...]
        rest = jnp.concatenate(
            [local[2 * quarter : 3 * quarter, 2 * quarter :], local[3 * quarter :, 2 * quarter :]], axis=1
        )
        rest = jnp.concatenate([local[quarter : 2 * quarter, :], rest], axis=0)
        for g, part in enumerate((local, rest)):
            pieces, plane, _, _ = groups[g]
            height = pieces.shape[1]
            for index in range(n_texel):
                pieces[index] = part[index * height : (index + 1) * height, :]
            for d in range(1, n_texel):
                copy(
                    pieces.at[texels[d]], plane.at[d], plane_send.at[g], plane_recv.at[g], (texels[d], light)
                ).start()

    def column_start():
        for g, (pieces, plane, column, _) in enumerate(groups):
            others = pl.ds(1, n_texel - 1)
            copy(pieces.at[others], plane.at[others], plane_send.at[g], plane_recv.at[g], (texels[1], light)).wait()
            total = pieces[texel]
            for d in range(1, n_texel):
                total = total + plane[d]
            column[own_column] = total
            for d in range(1, n_light):
                copy(
                    column.at[own_column], column.at[own_column], column_send.at[g], column_recv.at[g],
                    (texel, lights[d]),
                ).start()

    def rows_start(g, coming):
        _, _, column, rows = groups[g]
        some = column.at[pl.ds(0, coming)]
        copy(some, some, column_send.at[g], column_recv.at[g], (texel, lights[1])).wait_recv()
        total = column[0]
        for index in range(1, owners):
            total = total + column[index]
        rows[texel] = total
        for d in range(1, n_texel):
            copy(rows.at[texel], rows.at[texel], row_send.at[g], row_recv.at[g], (texels[d], light)).start()

    def column_sent():
        for g in range(2):
            sent = groups[g][1].at[pl.ds(0, n_light - 1)]
            copy(sent, sent, column_send.at[g], column_recv.at[g], (texel, lights[1])).wait_send()

    @pl.when(inner == 0)
    def _():
        done, held_back = 0, ends * 5 // 8
        for c in range(ends):
            rows = rows_at(0, c, CHUNK)
            sum_copy(0, c, inward).wait_recv()
            whole[rows, :] = partial_ref[rows, :] + landed[chunk_of(0, c)]
            if c == held_back:
                all_sent(sum_send, capacity // CHUNK - ends)
                for earlier in range(c):
                    back_copy(0, earlier, inward).start()
            if c >= held_back:
                back_copy(0, c, inward).start()
            if c + 1 in (ends // 2, ends * 5 // 6, ends):
                add_gram(0, done, c + 1 - done)
                done = c + 1
        plane_start()
        split_rows(0)
        column_start()
        for g in range(2):
            rows_start(g, owners - 1)

    @pl.when(inner == 1)
    def _():
        for kind, o, c in relay_order(shares):
            if kind == "plane":
                add_gram(1, 0, owned)
                plane_start()
            elif kind == "column":
                column_start()
            elif kind == "rows":
                rows_start(c, owners - 1 if owned else owners)
            elif kind == "final":
                near_copy(c, inward).wait_recv()
                sum_copy(1, c, inward).wait_recv()
                rows = rows_at(1, c, CHUNK)
                whole[rows, :] = partial_ref[rows, :] + near[c] + landed[chunk_of(1, c)]
                back_copy(1, c, inward).start()
                back_copy(1, c, outward).start()
            elif kind == "inward" or kind == "outward":
                going = sum_copy(o, c, inward if kind == "inward" else outward)
                going.wait_recv()
                rows = rows_at(o, c, CHUNK)
                partial_ref[rows, :] = partial_ref[rows, :] + landed[chunk_of(o, c)]
                going.start()
            else:
                going = back_copy(o, c, inward if kind == "back_inward" else outward)
                going.wait_recv()
                going.start()
        for o in range(n_light):
            split_rows(o)

    def row_whole(g):
        others = groups[g][3].at[pl.ds(1, n_texel - 1)]
        return copy(others, others, row_send.at[g], row_recv.at[g], (texels[1], light))

    valid = counts_ref[0]
    for index in range(1, n_texel):
        valid = valid + counts_ref[index]
    valid = valid.astype(jnp.float32)
    row_whole(0).wait_recv()
    height = rows_first.shape[1]
    for index in range(n_texel):
        work[index * height : (index + 1) * height, :size] = rows_first[index] / valid

    def finish_gram():
        row_whole(1).wait_recv()
        height = rows_rest.shape[1]
        rest = jnp.concatenate([rows_rest[index] for index in range(n_texel)], axis=0) / valid
        work[quarter : 2 * quarter, :size] = rest[:quarter, :]
        work[2 * quarter :, : 2 * quarter] = jnp.zeros((2 * quarter, 2 * quarter), jnp.float32)
        work[2 * quarter : 3 * quarter, 2 * quarter : size] = rest[quarter:, : 2 * quarter]
        work[3 * quarter :, 2 * quarter : size] = rest[quarter:, 2 * quarter :]

    def finish_rows():
        @pl.when(inner == 0)
        def _():
            for o in range(1, n_light):
                for c in range(shares[o]):
                    back_copy(o, c, inward).wait_recv()
                split_rows(o)

    factor_inverse(work, finish_gram, finish_rows)
    inverse = split(work[:, size:])
    half_ref[...] = product(inverse, (high[...], low[...])).astype(jnp.bfloat16)
    basis_out = pltpu.make_async_copy(basis_ref, basis_hbm, local_sems.at[0])

    def basis_rows(step):
        rows = slice(step * middle, (step + 1) * middle)
        basis_ref[rows, :] = product((high[rows, :], low[rows, :]), inverse)
        if step == 1:
            basis_out.start()

    scatter_sum(
        n_texel, half_ref, tile_ref, product_ref, coeffs_ref, valid, held, arrived, out_send, out_recv, basis_rows
    )
    coeffs_out = pltpu.make_async_copy(coeffs_ref, coeffs_hbm, local_sems.at[1])
    coeffs_out.start()
    for half in range(2):
        sent = held.at[half, pl.ds(0, n_texel - 1)]
        copy(sent, sent, out_send.at[half], out_recv.at[half, 0], (texels[1], light)).wait_send()

    @pl.when(inner == 0)
    def _():
        all_sent(back_send, ends)
        column_sent()

    @pl.when(inner == 1)
    def _():
        all_sent(sum_send, 2 * ends + owned)
        all_sent(back_send, 2 * ends + 3 * owned)
        if owned:
            column_sent()

    for g in range(2):
        row_whole(g).wait_send()
    basis_out.wait()
    coeffs_out.wait()


def halving_order(bits, last_first):
    rest = list(range(1, bits))
    return [0] + (rest[::-1] if last_first else rest)


def scatter_sum(n_texel, half_ref, tile_ref, partial_ref, out_ref, valid, held, landed, send_sem, recv_sem, meanwhile):
    texel, light = lax.axis_index("texel"), lax.axis_index("light")
    bits = n_texel.bit_length() - 1
    bit = [lax.rem(texel // (1 << b), 2) for b in range(bits)]
    partner = [texel + (1 - 2 * bit[b]) * (1 << b) for b in range(bits)]
    piece = partial_ref.shape[0] // n_texel
    width = partial_ref.shape[1] // 2

    def start_of(mask):
        block = 0
        for b in range(bits):
            flipped = 1 - bit[b] if mask >> b & 1 else bit[b]
            block = block + flipped * (1 << b)
        return pl.multiple_of(block * piece, piece)

    def multiply(half):
        columns = slice(half * width, (half + 1) * width)
        partial_ref[:, columns] = lax.dot_general(
            half_ref[...], tile_ref[:, columns], (((1,), (0,)), ((), ())), preferred_element_type=jnp.float32
        )

    orders = [halving_order(bits, False), halving_order(bits, True)]
    root = jnp.sqrt(jnp.full((piece, width), valid))
    flights = [{}, {}]
    used = [0, 0]
    for step in range(bits):
        for half, order in enumerate(orders):
            if step == 0:
                multiply(half)
            b = order[step]
            left = [m for m in range(n_texel) if all(not m >> done & 1 for done in order[:step])]
            later = order[step + 1 :]
            going = [m for m in left if m >> b & 1]
            going.sort(key=lambda m: [-(m >> c & 1) for c in later])
            columns = pl.ds(half * width, width)
            for m in going:
                kept = m - (1 << b)
                if step == 0:
                    source = partial_ref.at[pl.ds(start_of(m), piece), columns]
                else:
                    arrived = flights[half].pop((step - 1, m))
                    arrived.wait_recv()
                    below = (
                        partial_ref[pl.ds(start_of(m), piece), columns] if step == 1 else held[half, m]
                    )
                    held[half, m] = below + landed[half, step - 1, m]
                    source = held.at[half, m]
                copy = pltpu.make_async_remote_copy(
                    src_ref=source,
                    dst_ref=landed.at[half, step, kept],
                    send_sem=send_sem.at[half],
                    recv_sem=recv_sem.at[half, used[half]],
                    device_id=(partner[b], light),
                    device_id_type=MESH_ID,
                )
                copy.start()
                used[half] += 1
                flights[half][step, kept] = copy
        if step < 2:
            meanwhile(step)
        if step:
            for half, order in enumerate(orders):
                for key in [k for k in flights[half] if k[0] == step - 1]:
                    m = key[1]
                    flights[half].pop(key).wait_recv()
                    columns = pl.ds(half * width, width)
                    below = (
                        partial_ref[pl.ds(start_of(m), piece), columns] if step == 1 else held[half, m]
                    )
                    held[half, m] = below + landed[half, step - 1, m]
    for half in range(2):
        columns = pl.ds(half * width, width)
        flights[half].pop((bits - 1, 0)).wait_recv()
        below = partial_ref[pl.ds(start_of(0), piece), columns] if bits == 1 else held[half, 0]
        out_ref[:, half * width : (half + 1) * width] = (below + landed[half, bits - 1, 0]) / root


def write_out(basis_ref, coeffs_ref, basis_out, coeffs_out, sems):
    copies = [
        pltpu.make_async_copy(basis_ref, basis_out, sems.at[0]),
        pltpu.make_async_copy(coeffs_ref, coeffs_out, sems.at[1]),
    ]
    for going in copies:
        going.start()
    for going in copies:
        going.wait()


def on_device(n_texel, n_light, tex_feat, light_feat, sketch, row_counts):
    capacity, size = tex_feat.shape[0], sketch.shape[1]
    lights = light_feat.shape[0]
    block, step = capacity // 4, next(w for w in (256, 128) if lights % w == 0)
    shares, _ = layout_of(capacity, n_light)
    owners, piece = sum(1 for share in shares if share), size // n_texel
    first, rest = size // 4 // n_texel, size // 2 // n_texel
    width, bits = lights // 2, n_texel.bit_length() - 1
    vmem = pl.BlockSpec(memory_space=pltpu.VMEM)
    anywhere = pl.BlockSpec(memory_space=pl.ANY)
    f32, half = jnp.float32, jnp.bfloat16
    sems = pltpu.SemaphoreType.DMA
    basis, coeffs = pl.pallas_call(
        functools.partial(whole_step, n_texel, n_light),
        out_shape=(pltpu.VMEM((capacity, size), f32), pltpu.VMEM((piece, lights), f32)),
        in_specs=[anywhere] * 4,
        out_specs=(anywhere, anywhere),
        scratch_shapes=[
            pltpu.VMEM(tex_feat.shape, half),
            pltpu.VMEM(light_feat.shape, half),
            pltpu.VMEM(sketch.shape, half),
            pltpu.SMEM(row_counts.shape, jnp.int32),
            pltpu.VMEM((capacity, size), f32),
            pltpu.VMEM((piece, lights), f32),
            pltpu.VMEM((capacity, lights), half),
            pltpu.VMEM((size, capacity), half),
            pltpu.VMEM((size, lights), f32),
            pltpu.VMEM((2, n_texel, piece, width), f32),
            pltpu.VMEM((2, bits, n_texel, piece, width), f32),
            pltpu.VMEM((block, step), f32),
            pltpu.VMEM((block, step), f32),
            pltpu.VMEM((capacity, size), f32),
            pltpu.VMEM((capacity // CHUNK, CHUNK, size), f32),
            pltpu.VMEM((max(shares[1], 1), CHUNK, size), f32),
            pltpu.VMEM((capacity, size), f32),
            pltpu.VMEM((size, 2 * size), f32),
            pltpu.VMEM((size, size), f32),
            pltpu.VMEM((capacity, size), half),
            pltpu.VMEM((capacity, size), half),
            pltpu.VMEM((n_texel, first, size), f32), pltpu.VMEM((n_texel, rest, size), f32),
            pltpu.VMEM((n_texel, first, size), f32), pltpu.VMEM((n_texel, rest, size), f32),
            pltpu.VMEM((owners, first, size), f32), pltpu.VMEM((owners, rest, size), f32),
            pltpu.VMEM((n_texel, first, size), f32), pltpu.VMEM((n_texel, rest, size), f32),
            sems, sems, sems((capacity // CHUNK,)), sems((max(shares[1], 1),)),
            sems((2,)), sems((2,)),
            sems((2,)), sems((2,)),
            sems((2,)), sems((2,)),
            sems((2,)), sems((2, n_texel - 1)),
            sems((5,)), sems((5,)),
        ],
        compiler_params=pltpu.CompilerParams(collective_id=1, has_side_effects=True),
    )(tex_feat, light_feat, sketch, row_counts)
    return pl.pallas_call(
        write_out,
        out_shape=(jax.ShapeDtypeStruct((capacity, size), f32), jax.ShapeDtypeStruct((piece, lights), f32)),
        in_specs=[vmem, vmem],
        out_specs=(pl.BlockSpec(memory_space=pl.ANY),) * 2,
        scratch_shapes=[sems((2,))],
    )(*(pltpu.with_memory_space_constraint(x, pltpu.VMEM) for x in (basis, coeffs)))


def solution(mesh):
    placed = (P("texel", None), P("light", None), P("light", None), P())
    return jax.shard_map(
        functools.partial(on_device, mesh.shape["texel"], mesh.shape["light"]),
        mesh=mesh,
        in_specs=placed,
        out_specs=(P("texel", None), P("texel", "light")),
        check_vma=False,
    )
```

```python
import functools

import jax
import jax.numpy as jnp
from jax import lax
from jax.experimental import pallas as pl
from jax.experimental.pallas import tpu as pltpu
from jax.sharding import PartitionSpec as P

HIGHEST = lax.Precision.HIGHEST
BLOCK = 64
CHUNK = 16
INV_TWO_PI = 0.15915494309189535
SINE = (6.283185273788226, -41.34167747777608, 81.60223120329199, -76.57499125549666, 39.71091094809089)


def bounded_sine(x):
    turns = x * INV_TWO_PI - 0.25
    z = 0.25 - jnp.abs(turns - jnp.round(turns))
    s = z * z
    value = SINE[-1] * s + SINE[-2]
    for coefficient in SINE[-3::-1]:
        value = value * s + coefficient
    return value * z


def eliminate(block):
    rows = [block[8 * t : 8 * t + 8, :] for t in range(8)]
    below = lax.broadcasted_iota(jnp.int32, (8, 128), 0)

    def line_of(value, k):
        return jnp.broadcast_to(value[k : k + 1, :], (8, 128))

    def lane_of(value, k):
        return jnp.broadcast_to(value[:, k : k + 1], (8, 128))

    own = [lane_of(rows[0], k) for k in range(8)]
    for p in range(8):
        columns = {(t, k): lane_of(rows[t], 8 * p + k) for t in range(p + 1, 8) for k in range(8)}
        ahead = [lane_of(rows[p + 1], 8 * p + 8 + k) for k in range(8)] if p < 7 else None
        for k in range(8):
            inverse = 1.0 / line_of(own[k], k)
            factor = jnp.where(below > k, own[k] * inverse, 0.0)
            entries = {later: line_of(own[later], k) for later in range(k + 1, 8)}
            for later, entry in entries.items():
                own[later] = own[later] - factor * entry
            pivot_row = line_of(rows[p], k)
            rows[p] = rows[p] - factor * pivot_row
            for t in range(p + 1, 8):
                factor = columns[t, k] * inverse
                if t == p + 1:
                    for later in range(8):
                        ahead[later] = ahead[later] - factor * line_of(columns[t, k], later)
                for later, entry in entries.items():
                    columns[t, later] = columns[t, later] - factor * entry
                rows[t] = rows[t] - factor * pivot_row
        own = ahead
    return jnp.concatenate(rows, axis=0)


def factor_inverse(work_ref, finish_gram, finish_rows):
    size = work_ref.shape[0]
    row = lax.broadcasted_iota(jnp.int32, (size, size), 0)
    column = lax.broadcasted_iota(jnp.int32, (size, size), 1)
    work_ref[:, size:] = jnp.where(row == column, 1.0, 0.0).astype(jnp.float32)
    lane = lax.broadcasted_iota(jnp.int32, (BLOCK, 128), 1)
    line = lax.broadcasted_iota(jnp.int32, (BLOCK, 128), 0)
    for start in range(0, size, BLOCK):
        own = slice(start, start + BLOCK)
        first = start // 128 * 128
        last = size + (start + BLOCK + 127) // 128 * 128
        tile = work_ref[own, first : first + 128]
        if start % 128:
            tile = pltpu.roll(tile, 64, 1)
        unit = jnp.where(lane - BLOCK == line, 1.0, 0.0)
        done = eliminate(jnp.where(lane < BLOCK, tile, unit))
        pivots = jnp.sum(jnp.where(lane == line, done, 0.0), axis=1, keepdims=True)
        scaled = pltpu.roll(done * lax.rsqrt(pivots), 64, 1)[:, :BLOCK]
        both = jnp.dot(scaled, work_ref[own, first:last], precision=HIGHEST, preferred_element_type=jnp.float32)
        work_ref[own, size:last] = both[:, size - first :]
        if start == 0:
            finish_gram()
        if start == 2 * BLOCK:
            finish_rows()
        flipped = both[:, : size - first].T
        for lower in ((start + BLOCK, start + 2 * BLOCK), (start + 2 * BLOCK, size)):
            if lower[0] < min(lower[1], size):
                work_ref[lower[0] : lower[1], first:last] -= jnp.dot(
                    flipped[lower[0] - first : lower[1] - first, :], both,
                    precision=HIGHEST, preferred_element_type=jnp.float32,
                )


def split(value):
    high = value.astype(jnp.bfloat16)
    return high, (value - high.astype(jnp.float32)).astype(jnp.bfloat16)


def product(left, right):
    def one(a, b):
        return lax.dot_general(a, b, (((1,), (1,)), ((), ())), preferred_element_type=jnp.float32)

    return one(left[0], right[0]) + (one(left[0], right[1]) + one(left[1], right[0]))


MESH_ID = pl.DeviceIdType.MESH


def layout_of(capacity, n_light):
    count = capacity // CHUNK
    if n_light == 4:
        shares = [count * 3 // 8, count // 8, count // 8, count * 3 // 8]
    else:
        shares = [count // 2] + [0] * (n_light - 2) + [count // 2]
    return shares, [sum(shares[:z]) for z in range(n_light)]


def relay_order(shares):
    far, ends, owned = len(shares) - 1, shares[0], shares[1]
    outgoing = [(far, c) for c in range(ends)] + [(2, c) for c in range(owned)]
    hop = 8.3 if owned else 0.29 * ends
    last = ends + owned + 2 * hop
    events = [(i + hop, "inward", o, c) for i, (o, c) in enumerate(outgoing)]
    events += [(c + 2 * hop, "outward", 0, c) for c in range(ends)]
    if owned:
        events += [(ends + c + 2 * hop, "final", 1, c) for c in range(owned)]
        events += [(ends + c + 3 * hop, "back_outward", 2, c) for c in range(owned)]
        events += [(last + 0.5, "plane", 0, 0), (last + 12.5, "column", 0, 0)]
    events += [(last + 2 + c, "back_inward", 0, c) for c in range(ends)]
    events += [(last + 2 + hop + c, "back_outward", far, c) for c in range(ends)]
    events += [(last + 22 + 3 * g, "rows", 0, g) for g in range(2)]
    return [event[1:] for event in sorted(events)]


def whole_step(
    n_texel, n_light, tex_hbm, feat_hbm, sketch_hbm, counts_hbm, basis_ref, coeffs_ref,
    tex_ref, feat_ref, sketch_ref, counts_ref,
    tile_ref, half_ref, product_ref, held, arrived,
    logits_even, logits_odd, partial_ref,
    landed, near, whole, work, gram, high, low,
    pieces_first, pieces_rest, plane_first, plane_rest, column_first, column_rest, rows_first, rows_rest,
    sum_send, back_send, chunk_recv, near_recv,
    plane_send, plane_recv, column_send, column_recv, row_send, row_recv, out_send, out_recv,
    local_sems, tex_sems,
):
    texel, light = lax.axis_index("texel"), lax.axis_index("light")
    capacity, size = partial_ref.shape
    width = logits_even.shape[1]
    block = logits_even.shape[0]
    middle = capacity // 2
    shares, starts = layout_of(capacity, n_light)
    far, ends, owned = n_light - 1, shares[0], shares[1]
    owners = column_first.shape[0]
    upper = light // (n_light // 2)

    def chunk_of(o, c):
        return starts[o] + c + upper * (starts[far - o] - starts[o])

    def rows_at(o, c, height):
        return pl.ds(pl.multiple_of(chunk_of(o, c) * CHUNK, CHUNK), height)

    half_block = block // 2
    per_half = half_block // CHUNK
    turns = [(rows_at(far, 0, half_block), half_block, [(far, c) for c in range(per_half)])]
    if owned:
        turns += [(rows_at(far, per_half, block), block, [(far, c) for c in range(per_half, ends)])]
        shared = pl.ds(starts[1] * CHUNK, block)
        turns += [(shared, block, [(o, c) for o in (2, 1) for c in range(owned)])]
        turns += [(rows_at(0, 0, block), block, []), (rows_at(0, 2 * per_half, half_block), half_block, [])]
    else:
        turns += [(rows_at(far, per_half, half_block), half_block, [(far, per_half + c) for c in range(per_half)])]
        turns += [(rows_at(far, 2 * per_half, block), block, [(far, c) for c in range(2 * per_half, ends)])]
        turns += [(rows_at(0, 0, block), block, []), (rows_at(0, 2 * per_half, block), block, [])]

    tex_copies = [
        pltpu.make_async_copy(tex_hbm.at[rows], tex_ref.at[rows], tex_sems.at[index])
        for index, (rows, _, _) in enumerate(turns)
    ]
    feat_half = feat_ref.shape[0] // width // 2
    feat_copies = [
        pltpu.make_async_copy(
            feat_hbm.at[pl.ds(c * width, width)], feat_ref.at[pl.ds(c * width, width)],
            local_sems.at[2 + c // feat_half],
        )
        for c in range(feat_ref.shape[0] // width)
    ]
    sketch_copy = pltpu.make_async_copy(sketch_hbm, sketch_ref, local_sems.at[0])
    counts_copy = pltpu.make_async_copy(counts_hbm, counts_ref, local_sems.at[1])
    for going in tex_copies[:1] + feat_copies + [counts_copy, sketch_copy]:
        going.start()
    lights = [lax.rem(light + d, n_light) for d in range(n_light)]
    texels = [lax.rem(texel + d, n_texel) for d in range(n_texel)]
    depth = light + upper * (n_light - 1 - 2 * light)
    inner = 1 - (n_light // 2 - depth) // (n_light // 2)
    inward, outward = light + 1 - 2 * upper, light - 1 + 2 * upper

    barrier = pltpu.get_barrier_semaphore()
    peers = [(texel, lights[d]) for d in range(1, n_light)] + [(texels[d], light) for d in range(1, n_texel)]
    for peer in peers:
        pl.semaphore_signal(barrier, inc=1, device_id=peer, device_id_type=MESH_ID)

    def copy(source, target, send_sem, recv_sem, device):
        return pltpu.make_async_remote_copy(
            src_ref=source, dst_ref=target, send_sem=send_sem, recv_sem=recv_sem,
            device_id=device, device_id_type=MESH_ID,
        )

    def sum_copy(o, c, to):
        chunk = chunk_of(o, c)
        return copy(
            partial_ref.at[rows_at(o, c, CHUNK)], landed.at[chunk], sum_send, chunk_recv.at[chunk], (texel, to)
        )

    def near_copy(c, to):
        return copy(partial_ref.at[rows_at(1, c, CHUNK)], near.at[c], sum_send, near_recv.at[c], (texel, to))

    def back_copy(o, c, to):
        rows = rows_at(o, c, CHUNK)
        return copy(whole.at[rows], whole.at[rows], back_send, chunk_recv.at[chunk_of(o, c)], (texel, to))

    def all_sent(sem, chunks):
        while chunks:
            some = min(chunks, capacity // CHUNK)
            sent = whole.at[pl.ds(0, some * CHUNK)]
            copy(sent, sent, sem, chunk_recv.at[0], (texel, inward)).wait_send()
            chunks -= some

    def fill(turn):
        rows, height, _ = turns[turn]
        logits = (logits_even.at[pl.ds(0, height)], logits_odd.at[pl.ds(0, height)])
        count = feat_ref.shape[0] // width

        def feat_wait(part):
            rows = pl.ds(part * feat_half * width, feat_half * width)
            pltpu.make_async_copy(feat_hbm.at[rows], feat_ref.at[rows], local_sems.at[2 + part]).wait()

        def product_of(c):
            if turn == 0 and c == feat_half:
                feat_wait(1)
                for going in tex_copies[1:]:
                    going.start()
            return lax.dot_general(
                tex_ref[rows, :], feat_ref[c * width : (c + 1) * width, :], (((1,), (1,)), ((), ())),
                preferred_element_type=jnp.float32,
            )

        tex_copies[turn].wait()
        if turn == 0:
            feat_wait(0)
        logits[0][...] = product_of(0)
        for c in range(count):
            if c + 1 < count:
                logits[(c + 1) % 2][...] = product_of(c + 1)
            tile_ref[rows, c * width : (c + 1) * width] = bounded_sine(logits[c % 2][...]).astype(jnp.bfloat16)
        if turn == 0:
            sketch_copy.wait()
            counts_copy.wait()
        own_count = counts_ref[texel]
        slot = rows.start + lax.broadcasted_iota(jnp.int32, (height, size), 0)
        sums = jnp.dot(tile_ref[rows, :], sketch_ref[...], preferred_element_type=jnp.float32)
        partial_ref[rows, :] = jnp.where(slot < own_count, sums, 0.0)

    for turn, (_, _, ready) in enumerate(turns):
        fill(turn)
        if turn == 0:
            pl.semaphore_wait(barrier, len(peers))

        @pl.when(inner == 0)
        def _():
            for o, c in ready:
                (near_copy(c, inward) if o == 1 and owned else sum_copy(o, c, inward)).start()

    def split_rows(o):
        if shares[o]:
            rows = rows_at(o, 0, shares[o] * CHUNK)
            high[rows, :], low[rows, :] = split(whole[rows, :])

    groups = (
        (pieces_first, plane_first, column_first, rows_first),
        (pieces_rest, plane_rest, column_rest, rows_rest),
    )
    quarter = size // 4
    own_column = light if owned else upper

    def add_gram(o, first, chunks):
        own = whole[rows_at(o, first, chunks * CHUNK), :]
        some = lax.dot_general(
            own, own, (((0,), (0,)), ((), ())), precision=HIGHEST, preferred_element_type=jnp.float32
        )
        gram[...] = gram[...] + some if first else some

    def plane_start():
        local = gram[...]
        rest = jnp.concatenate(
            [local[2 * quarter : 3 * quarter, 2 * quarter :], local[3 * quarter :, 2 * quarter :]], axis=1
        )
        rest = jnp.concatenate([local[quarter : 2 * quarter, :], rest], axis=0)
        for g, part in enumerate((local, rest)):
            pieces, plane, _, _ = groups[g]
            height = pieces.shape[1]
            for index in range(n_texel):
                pieces[index] = part[index * height : (index + 1) * height, :]
            for d in range(1, n_texel):
                copy(
                    pieces.at[texels[d]], plane.at[d], plane_send.at[g], plane_recv.at[g], (texels[d], light)
                ).start()

    def column_start():
        for g, (pieces, plane, column, _) in enumerate(groups):
            others = pl.ds(1, n_texel - 1)
            copy(pieces.at[others], plane.at[others], plane_send.at[g], plane_recv.at[g], (texels[1], light)).wait()
            total = pieces[texel]
            for d in range(1, n_texel):
                total = total + plane[d]
            column[own_column] = total
            for d in range(1, n_light):
                copy(
                    column.at[own_column], column.at[own_column], column_send.at[g], column_recv.at[g],
                    (texel, lights[d]),
                ).start()

    def rows_start(g, coming):
        _, _, column, rows = groups[g]
        some = column.at[pl.ds(0, coming)]
        copy(some, some, column_send.at[g], column_recv.at[g], (texel, lights[1])).wait_recv()
        total = column[0]
        for index in range(1, owners):
            total = total + column[index]
        rows[texel] = total
        for d in range(1, n_texel):
            copy(rows.at[texel], rows.at[texel], row_send.at[g], row_recv.at[g], (texels[d], light)).start()

    def column_sent():
        for g in range(2):
            sent = groups[g][1].at[pl.ds(0, n_light - 1)]
            copy(sent, sent, column_send.at[g], column_recv.at[g], (texel, lights[1])).wait_send()

    @pl.when(inner == 0)
    def _():
        done, held_back = 0, ends * 5 // 8
        for c in range(ends):
            rows = rows_at(0, c, CHUNK)
            sum_copy(0, c, inward).wait_recv()
            whole[rows, :] = partial_ref[rows, :] + landed[chunk_of(0, c)]
            if c == held_back:
                all_sent(sum_send, capacity // CHUNK - ends)
                for earlier in range(c):
                    back_copy(0, earlier, inward).start()
            if c >= held_back:
                back_copy(0, c, inward).start()
            if c + 1 in (ends // 2, ends * 5 // 6, ends):
                add_gram(0, done, c + 1 - done)
                done = c + 1
        plane_start()
        split_rows(0)
        column_start()
        for g in range(2):
            rows_start(g, owners - 1)

    @pl.when(inner == 1)
    def _():
        for kind, o, c in relay_order(shares):
            if kind == "plane":
                add_gram(1, 0, owned)
                plane_start()
            elif kind == "column":
                column_start()
            elif kind == "rows":
                rows_start(c, owners - 1 if owned else owners)
            elif kind == "final":
                near_copy(c, inward).wait_recv()
                sum_copy(1, c, inward).wait_recv()
                rows = rows_at(1, c, CHUNK)
                whole[rows, :] = partial_ref[rows, :] + near[c] + landed[chunk_of(1, c)]
                back_copy(1, c, inward).start()
                back_copy(1, c, outward).start()
            elif kind == "inward" or kind == "outward":
                going = sum_copy(o, c, inward if kind == "inward" else outward)
                going.wait_recv()
                rows = rows_at(o, c, CHUNK)
                partial_ref[rows, :] = partial_ref[rows, :] + landed[chunk_of(o, c)]
                going.start()
            else:
                going = back_copy(o, c, inward if kind == "back_inward" else outward)
                going.wait_recv()
                going.start()
        for o in range(n_light):
            split_rows(o)

    def row_whole(g):
        others = groups[g][3].at[pl.ds(1, n_texel - 1)]
        return copy(others, others, row_send.at[g], row_recv.at[g], (texels[1], light))

    valid = counts_ref[0]
    for index in range(1, n_texel):
        valid = valid + counts_ref[index]
    valid = valid.astype(jnp.float32)
    row_whole(0).wait_recv()
    height = rows_first.shape[1]
    for index in range(n_texel):
        work[index * height : (index + 1) * height, :size] = rows_first[index] / valid

    def finish_gram():
        row_whole(1).wait_recv()
        height = rows_rest.shape[1]
        rest = jnp.concatenate([rows_rest[index] for index in range(n_texel)], axis=0) / valid
        work[quarter : 2 * quarter, :size] = rest[:quarter, :]
        work[2 * quarter :, : 2 * quarter] = jnp.zeros((2 * quarter, 2 * quarter), jnp.float32)
        work[2 * quarter : 3 * quarter, 2 * quarter : size] = rest[quarter:, : 2 * quarter]
        work[3 * quarter :, 2 * quarter : size] = rest[quarter:, 2 * quarter :]

    def finish_rows():
        @pl.when(inner == 0)
        def _():
            for o in range(1, n_light):
                for c in range(shares[o]):
                    back_copy(o, c, inward).wait_recv()
                split_rows(o)

    factor_inverse(work, finish_gram, finish_rows)
    inverse = split(work[:, size:])
    half_ref[...] = product(inverse, (high[...], low[...])).astype(jnp.bfloat16)

    def basis_rows(step):
        rows = slice(step * middle, (step + 1) * middle)
        basis_ref[rows, :] = product((high[rows, :], low[rows, :]), inverse)

    scatter_sum(
        n_texel, half_ref, tile_ref, product_ref, coeffs_ref, valid, held, arrived, out_send, out_recv, basis_rows
    )
    for half in range(2):
        sent = held.at[half, pl.ds(0, n_texel - 1)]
        copy(sent, sent, out_send.at[half], out_recv.at[half, 0], (texels[1], light)).wait_send()

    @pl.when(inner == 0)
    def _():
        all_sent(back_send, ends)
        column_sent()

    @pl.when(inner == 1)
    def _():
        all_sent(sum_send, 2 * ends + owned)
        all_sent(back_send, 2 * ends + 3 * owned)
        if owned:
            column_sent()

    for g in range(2):
        row_whole(g).wait_send()


def halving_order(bits, last_first):
    rest = list(range(1, bits))
    return [0] + (rest[::-1] if last_first else rest)


def scatter_sum(n_texel, half_ref, tile_ref, partial_ref, out_ref, valid, held, landed, send_sem, recv_sem, meanwhile):
    texel, light = lax.axis_index("texel"), lax.axis_index("light")
    bits = n_texel.bit_length() - 1
    bit = [lax.rem(texel // (1 << b), 2) for b in range(bits)]
    partner = [texel + (1 - 2 * bit[b]) * (1 << b) for b in range(bits)]
    piece = partial_ref.shape[0] // n_texel
    width = partial_ref.shape[1] // 2

    def start_of(mask):
        block = 0
        for b in range(bits):
            flipped = 1 - bit[b] if mask >> b & 1 else bit[b]
            block = block + flipped * (1 << b)
        return pl.multiple_of(block * piece, piece)

    def multiply(half):
        columns = slice(half * width, (half + 1) * width)
        partial_ref[:, columns] = lax.dot_general(
            half_ref[...], tile_ref[:, columns], (((1,), (0,)), ((), ())), preferred_element_type=jnp.float32
        )

    orders = [halving_order(bits, False), halving_order(bits, True)]
    root = jnp.sqrt(jnp.full((piece, width), valid))
    flights = [{}, {}]
    used = [0, 0]
    for step in range(bits):
        for half, order in enumerate(orders):
            if step == 0:
                multiply(half)
            b = order[step]
            left = [m for m in range(n_texel) if all(not m >> done & 1 for done in order[:step])]
            later = order[step + 1 :]
            going = [m for m in left if m >> b & 1]
            going.sort(key=lambda m: [-(m >> c & 1) for c in later])
            columns = pl.ds(half * width, width)
            for m in going:
                kept = m - (1 << b)
                if step == 0:
                    source = partial_ref.at[pl.ds(start_of(m), piece), columns]
                else:
                    arrived = flights[half].pop((step - 1, m))
                    arrived.wait_recv()
                    below = (
                        partial_ref[pl.ds(start_of(m), piece), columns] if step == 1 else held[half, m]
                    )
                    held[half, m] = below + landed[half, step - 1, m]
                    source = held.at[half, m]
                copy = pltpu.make_async_remote_copy(
                    src_ref=source,
                    dst_ref=landed.at[half, step, kept],
                    send_sem=send_sem.at[half],
                    recv_sem=recv_sem.at[half, used[half]],
                    device_id=(partner[b], light),
                    device_id_type=MESH_ID,
                )
                copy.start()
                used[half] += 1
                flights[half][step, kept] = copy
        if step < 2:
            meanwhile(step)
        if step:
            for half, order in enumerate(orders):
                for key in [k for k in flights[half] if k[0] == step - 1]:
                    m = key[1]
                    flights[half].pop(key).wait_recv()
                    columns = pl.ds(half * width, width)
                    below = (
                        partial_ref[pl.ds(start_of(m), piece), columns] if step == 1 else held[half, m]
                    )
                    held[half, m] = below + landed[half, step - 1, m]
    for half in range(2):
        columns = pl.ds(half * width, width)
        flights[half].pop((bits - 1, 0)).wait_recv()
        below = partial_ref[pl.ds(start_of(0), piece), columns] if bits == 1 else held[half, 0]
        out_ref[:, half * width : (half + 1) * width] = (below + landed[half, bits - 1, 0]) / root


def write_out(basis_ref, coeffs_ref, basis_out, coeffs_out, sems):
    parts = sems.shape[0] - 1
    height = basis_ref.shape[0] // parts
    copies = [pltpu.make_async_copy(coeffs_ref, coeffs_out, sems.at[parts])]
    for index in range(parts):
        rows = pl.ds(index * height, height)
        copies.append(pltpu.make_async_copy(basis_ref.at[rows], basis_out.at[rows], sems.at[index]))
    for going in copies:
        going.start()
    for going in copies:
        going.wait()


def on_device(n_texel, n_light, tex_feat, light_feat, sketch, row_counts):
    capacity, size = tex_feat.shape[0], sketch.shape[1]
    lights = light_feat.shape[0]
    block, step = capacity // 4, next(w for w in (256, 128) if lights % w == 0)
    shares, _ = layout_of(capacity, n_light)
    owners, piece = sum(1 for share in shares if share), size // n_texel
    first, rest = size // 4 // n_texel, size // 2 // n_texel
    width, bits = lights // 2, n_texel.bit_length() - 1
    vmem = pl.BlockSpec(memory_space=pltpu.VMEM)
    anywhere = pl.BlockSpec(memory_space=pl.ANY)
    f32, half = jnp.float32, jnp.bfloat16
    sems = pltpu.SemaphoreType.DMA
    basis, coeffs = pl.pallas_call(
        functools.partial(whole_step, n_texel, n_light),
        out_shape=(pltpu.VMEM((capacity, size), f32), pltpu.VMEM((piece, lights), f32)),
        in_specs=[anywhere] * 4,
        out_specs=(vmem, vmem),
        scratch_shapes=[
            pltpu.VMEM(tex_feat.shape, half),
            pltpu.VMEM(light_feat.shape, half),
            pltpu.VMEM(sketch.shape, half),
            pltpu.SMEM(row_counts.shape, jnp.int32),
            pltpu.VMEM((capacity, lights), half),
            pltpu.VMEM((size, capacity), half),
            pltpu.VMEM((size, lights), f32),
            pltpu.VMEM((2, n_texel, piece, width), f32),
            pltpu.VMEM((2, bits, n_texel, piece, width), f32),
            pltpu.VMEM((block, step), f32),
            pltpu.VMEM((block, step), f32),
            pltpu.VMEM((capacity, size), f32),
            pltpu.VMEM((capacity // CHUNK, CHUNK, size), f32),
            pltpu.VMEM((max(shares[1], 1), CHUNK, size), f32),
            pltpu.VMEM((capacity, size), f32),
            pltpu.VMEM((size, 2 * size), f32),
            pltpu.VMEM((size, size), f32),
            pltpu.VMEM((capacity, size), half),
            pltpu.VMEM((capacity, size), half),
            pltpu.VMEM((n_texel, first, size), f32), pltpu.VMEM((n_texel, rest, size), f32),
            pltpu.VMEM((n_texel, first, size), f32), pltpu.VMEM((n_texel, rest, size), f32),
            pltpu.VMEM((owners, first, size), f32), pltpu.VMEM((owners, rest, size), f32),
            pltpu.VMEM((n_texel, first, size), f32), pltpu.VMEM((n_texel, rest, size), f32),
            sems, sems, sems((capacity // CHUNK,)), sems((max(shares[1], 1),)),
            sems((2,)), sems((2,)),
            sems((2,)), sems((2,)),
            sems((2,)), sems((2,)),
            sems((2,)), sems((2, n_texel - 1)),
            sems((4,)), sems((5,)),
        ],
        compiler_params=pltpu.CompilerParams(collective_id=1, has_side_effects=True),
    )(tex_feat, light_feat, sketch, row_counts)
    return pl.pallas_call(
        write_out,
        out_shape=(jax.ShapeDtypeStruct((capacity, size), f32), jax.ShapeDtypeStruct((piece, lights), f32)),
        in_specs=[vmem, vmem],
        out_specs=(pl.BlockSpec(memory_space=pl.ANY),) * 2,
        scratch_shapes=[sems((5,))],
    )(*(pltpu.with_memory_space_constraint(x, pltpu.VMEM) for x in (basis, coeffs)))


def solution(mesh):
    placed = (P("texel", None), P("light", None), P("light", None), P())
    return jax.shard_map(
        functools.partial(on_device, mesh.shape["texel"], mesh.shape["light"]),
        mesh=mesh,
        in_specs=placed,
        out_specs=(P("texel", None), P("texel", "light")),
        check_vma=False,
    )
```

```python
import functools

import jax
import jax.numpy as jnp
from jax import lax
from jax.experimental import pallas as pl
from jax.experimental.pallas import tpu as pltpu
from jax.sharding import PartitionSpec as P

HIGHEST = lax.Precision.HIGHEST
BLOCK = 64
CHUNK = 16
INV_TWO_PI = 0.15915494309189535
SINE = (6.283185273788226, -41.34167747777608, 81.60223120329199, -76.57499125549666, 39.71091094809089)


def bounded_sine(x):
    turns = x * INV_TWO_PI - 0.25
    z = 0.25 - jnp.abs(turns - jnp.round(turns))
    s = z * z
    value = SINE[-1] * s + SINE[-2]
    for coefficient in SINE[-3::-1]:
        value = value * s + coefficient
    return value * z


def eliminate(block):
    rows = [block[8 * t : 8 * t + 8, :] for t in range(8)]
    below = lax.broadcasted_iota(jnp.int32, (8, 128), 0)

    def line_of(value, k):
        return jnp.broadcast_to(value[k : k + 1, :], (8, 128))

    def lane_of(value, k):
        return jnp.broadcast_to(value[:, k : k + 1], (8, 128))

    own = [lane_of(rows[0], k) for k in range(8)]
    for p in range(8):
        columns = {(t, k): lane_of(rows[t], 8 * p + k) for t in range(p + 1, 8) for k in range(8)}
        ahead = [lane_of(rows[p + 1], 8 * p + 8 + k) for k in range(8)] if p < 7 else None
        for k in range(8):
            inverse = 1.0 / line_of(own[k], k)
            factor = jnp.where(below > k, own[k] * inverse, 0.0)
            entries = {later: line_of(own[later], k) for later in range(k + 1, 8)}
            for later, entry in entries.items():
                own[later] = own[later] - factor * entry
            pivot_row = line_of(rows[p], k)
            rows[p] = rows[p] - factor * pivot_row
            for t in range(p + 1, 8):
                factor = columns[t, k] * inverse
                if t == p + 1:
                    for later in range(8):
                        ahead[later] = ahead[later] - factor * line_of(columns[t, k], later)
                for later, entry in entries.items():
                    columns[t, later] = columns[t, later] - factor * entry
                rows[t] = rows[t] - factor * pivot_row
        own = ahead
    return jnp.concatenate(rows, axis=0)


def factor_inverse(work_ref, finish_gram, finish_rows):
    size = work_ref.shape[0]
    row = lax.broadcasted_iota(jnp.int32, (size, size), 0)
    column = lax.broadcasted_iota(jnp.int32, (size, size), 1)
    work_ref[:, size:] = jnp.where(row == column, 1.0, 0.0).astype(jnp.float32)
    lane = lax.broadcasted_iota(jnp.int32, (BLOCK, 128), 1)
    line = lax.broadcasted_iota(jnp.int32, (BLOCK, 128), 0)
    for start in range(0, size, BLOCK):
        own = slice(start, start + BLOCK)
        first = start // 128 * 128
        last = size + (start + BLOCK + 127) // 128 * 128
        tile = work_ref[own, first : first + 128]
        if start % 128:
            tile = pltpu.roll(tile, 64, 1)
        unit = jnp.where(lane - BLOCK == line, 1.0, 0.0)
        done = eliminate(jnp.where(lane < BLOCK, tile, unit))
        pivots = jnp.sum(jnp.where(lane == line, done, 0.0), axis=1, keepdims=True)
        scaled = pltpu.roll(done * lax.rsqrt(pivots), 64, 1)[:, :BLOCK]
        both = jnp.dot(scaled, work_ref[own, first:last], precision=HIGHEST, preferred_element_type=jnp.float32)
        work_ref[own, size:last] = both[:, size - first :]
        if start == 0:
            finish_gram()
        if start == 2 * BLOCK:
            finish_rows()
        flipped = both[:, : size - first].T
        for lower in ((start + BLOCK, start + 2 * BLOCK), (start + 2 * BLOCK, size)):
            if lower[0] < min(lower[1], size):
                work_ref[lower[0] : lower[1], first:last] -= jnp.dot(
                    flipped[lower[0] - first : lower[1] - first, :], both,
                    precision=HIGHEST, preferred_element_type=jnp.float32,
                )


def split(value):
    high = value.astype(jnp.bfloat16)
    return high, (value - high.astype(jnp.float32)).astype(jnp.bfloat16)


def product(left, right):
    def one(a, b):
        return lax.dot_general(a, b, (((1,), (1,)), ((), ())), preferred_element_type=jnp.float32)

    return one(left[0], right[0]) + (one(left[0], right[1]) + one(left[1], right[0]))


MESH_ID = pl.DeviceIdType.MESH


def layout_of(capacity, n_light):
    count = capacity // CHUNK
    if n_light == 4:
        shares = [count * 3 // 8, count // 8, count // 8, count * 3 // 8]
    else:
        shares = [count // 2] + [0] * (n_light - 2) + [count // 2]
    return shares, [sum(shares[:z]) for z in range(n_light)]


def relay_order(shares):
    far, ends, owned = len(shares) - 1, shares[0], shares[1]
    outgoing = [(far, c) for c in range(ends)] + [(2, c) for c in range(owned)]
    hop = 8.3 if owned else 0.29 * ends
    last = ends + owned + 2 * hop
    events = [(i + hop, "inward", o, c) for i, (o, c) in enumerate(outgoing)]
    events += [(c + 2 * hop, "outward", 0, c) for c in range(ends)]
    if owned:
        events += [(ends + c + 2 * hop, "final", 1, c) for c in range(owned)]
        events += [(ends + c + 3 * hop, "back_outward", 2, c) for c in range(owned)]
        events += [(last + 0.5, "plane", 0, 0), (last + 12.5, "column", 0, 0)]
    events += [(last + 2 + c, "back_inward", 0, c) for c in range(ends)]
    events += [(last + 2 + hop + c, "back_outward", far, c) for c in range(ends)]
    events += [(last + 22 + 3 * g, "rows", 0, g) for g in range(2)]
    return [event[1:] for event in sorted(events)]


def whole_step(
    n_texel, n_light, tex_hbm, feat_hbm, sketch_hbm, counts_hbm, basis_ref, coeffs_ref,
    tex_ref, feat_ref, sketch_ref, counts_ref,
    tile_ref, half_ref, product_ref, held, arrived,
    logits_even, logits_odd, partial_ref,
    landed, near, whole, work, gram, high, low,
    pieces_first, pieces_rest, plane_first, plane_rest, column_first, column_rest, rows_first, rows_rest,
    sum_send, back_send, chunk_recv, near_recv,
    plane_send, plane_recv, column_send, column_recv, row_send, row_recv, out_send, out_recv,
    local_sems, tex_sems,
):
    texel, light = lax.axis_index("texel"), lax.axis_index("light")
    capacity, size = partial_ref.shape
    width = logits_even.shape[1]
    block = logits_even.shape[0]
    middle = capacity // 2
    shares, starts = layout_of(capacity, n_light)
    far, ends, owned = n_light - 1, shares[0], shares[1]
    owners = column_first.shape[0]
    upper = light // (n_light // 2)

    def chunk_of(o, c):
        return starts[o] + c + upper * (starts[far - o] - starts[o])

    def rows_at(o, c, height):
        return pl.ds(pl.multiple_of(chunk_of(o, c) * CHUNK, CHUNK), height)

    half_block = block // 2
    per_half = half_block // CHUNK
    turns = [(rows_at(far, 0, half_block), half_block, [(far, c) for c in range(per_half)])]
    if owned:
        turns += [(rows_at(far, per_half, block), block, [(far, c) for c in range(per_half, ends)])]
        shared = pl.ds(starts[1] * CHUNK, block)
        turns += [(shared, block, [(o, c) for o in (2, 1) for c in range(owned)])]
        turns += [(rows_at(0, 0, block), block, []), (rows_at(0, 2 * per_half, half_block), half_block, [])]
    else:
        turns += [(rows_at(far, per_half, half_block), half_block, [(far, per_half + c) for c in range(per_half)])]
        turns += [(rows_at(far, 2 * per_half, block), block, [(far, c) for c in range(2 * per_half, ends)])]
        turns += [(rows_at(0, 0, block), block, []), (rows_at(0, 2 * per_half, block), block, [])]

    tex_copies = [
        pltpu.make_async_copy(tex_hbm.at[rows], tex_ref.at[rows], tex_sems.at[index])
        for index, (rows, _, _) in enumerate(turns)
    ]
    feat_half = feat_ref.shape[0] // width // 2
    feat_copies = [
        pltpu.make_async_copy(
            feat_hbm.at[pl.ds(c * width, width)], feat_ref.at[pl.ds(c * width, width)],
            local_sems.at[2 + c // feat_half],
        )
        for c in range(feat_ref.shape[0] // width)
    ]
    sketch_copy = pltpu.make_async_copy(sketch_hbm, sketch_ref, local_sems.at[0])
    counts_copy = pltpu.make_async_copy(counts_hbm, counts_ref, local_sems.at[1])
    for going in tex_copies[:1] + feat_copies + [counts_copy, sketch_copy]:
        going.start()
    lights = [lax.rem(light + d, n_light) for d in range(n_light)]
    texels = [lax.rem(texel + d, n_texel) for d in range(n_texel)]
    depth = light + upper * (n_light - 1 - 2 * light)
    inner = 1 - (n_light // 2 - depth) // (n_light // 2)
    inward, outward = light + 1 - 2 * upper, light - 1 + 2 * upper

    barrier = pltpu.get_barrier_semaphore()
    peers = [(texel, lights[d]) for d in range(1, n_light)] + [(texels[d], light) for d in range(1, n_texel)]
    for peer in peers:
        pl.semaphore_signal(barrier, inc=1, device_id=peer, device_id_type=MESH_ID)

    def copy(source, target, send_sem, recv_sem, device):
        return pltpu.make_async_remote_copy(
            src_ref=source, dst_ref=target, send_sem=send_sem, recv_sem=recv_sem,
            device_id=device, device_id_type=MESH_ID,
        )

    def sum_copy(o, c, to):
        chunk = chunk_of(o, c)
        return copy(
            partial_ref.at[rows_at(o, c, CHUNK)], landed.at[chunk], sum_send, chunk_recv.at[chunk], (texel, to)
        )

    def near_copy(c, to):
        return copy(partial_ref.at[rows_at(1, c, CHUNK)], near.at[c], sum_send, near_recv, (texel, to))

    def back_copy(o, c, to):
        rows = rows_at(o, c, CHUNK)
        return copy(whole.at[rows], whole.at[rows], back_send, chunk_recv.at[chunk_of(o, c)], (texel, to))

    def all_sent(sem, chunks):
        while chunks:
            some = min(chunks, capacity // CHUNK)
            sent = whole.at[pl.ds(0, some * CHUNK)]
            copy(sent, sent, sem, chunk_recv.at[0], (texel, inward)).wait_send()
            chunks -= some

    def fill(turn):
        rows, height, _ = turns[turn]
        logits = (logits_even.at[pl.ds(0, height)], logits_odd.at[pl.ds(0, height)])
        count = feat_ref.shape[0] // width

        def feat_wait(part):
            rows = pl.ds(part * feat_half * width, feat_half * width)
            pltpu.make_async_copy(feat_hbm.at[rows], feat_ref.at[rows], local_sems.at[2 + part]).wait()

        def product_of(c):
            if turn == 0 and c == feat_half:
                feat_wait(1)
                for going in tex_copies[1:]:
                    going.start()
            return lax.dot_general(
                tex_ref[rows, :], feat_ref[c * width : (c + 1) * width, :], (((1,), (1,)), ((), ())),
                preferred_element_type=jnp.float32,
            )

        tex_copies[turn].wait()
        if turn == 0:
            feat_wait(0)
        logits[0][...] = product_of(0)
        for c in range(count):
            if c + 1 < count:
                logits[(c + 1) % 2][...] = product_of(c + 1)
            tile_ref[rows, c * width : (c + 1) * width] = bounded_sine(logits[c % 2][...]).astype(jnp.bfloat16)
        if turn == 0:
            sketch_copy.wait()
            counts_copy.wait()
        own_count = counts_ref[texel]
        slot = rows.start + lax.broadcasted_iota(jnp.int32, (height, size), 0)
        sums = jnp.dot(tile_ref[rows, :], sketch_ref[...], preferred_element_type=jnp.float32)
        partial_ref[rows, :] = jnp.where(slot < own_count, sums, 0.0)

    for turn, (_, _, ready) in enumerate(turns):
        fill(turn)
        if turn == 0:
            pl.semaphore_wait(barrier, len(peers))

        @pl.when(inner == 0)
        def _():
            for o, c in ready:
                (near_copy(c, inward) if o == 1 and owned else sum_copy(o, c, inward)).start()

    def split_rows(o):
        if shares[o]:
            rows = rows_at(o, 0, shares[o] * CHUNK)
            high[rows, :], low[rows, :] = split(whole[rows, :])

    groups = (
        (pieces_first, plane_first, column_first, rows_first),
        (pieces_rest, plane_rest, column_rest, rows_rest),
    )
    quarter = size // 4
    own_column = light if owned else upper

    def add_gram(o, first, chunks):
        own = whole[rows_at(o, first, chunks * CHUNK), :]
        some = lax.dot_general(
            own, own, (((0,), (0,)), ((), ())), precision=HIGHEST, preferred_element_type=jnp.float32
        )
        gram[...] = gram[...] + some if first else some

    def plane_start():
        local = gram[...]
        rest = jnp.concatenate(
            [local[2 * quarter : 3 * quarter, 2 * quarter :], local[3 * quarter :, 2 * quarter :]], axis=1
        )
        rest = jnp.concatenate([local[quarter : 2 * quarter, :], rest], axis=0)
        for g, part in enumerate((local, rest)):
            pieces, plane, _, _ = groups[g]
            height = pieces.shape[1]
            for index in range(n_texel):
                pieces[index] = part[index * height : (index + 1) * height, :]
            for d in range(1, n_texel):
                copy(
                    pieces.at[texels[d]], plane.at[d], plane_send.at[g], plane_recv.at[g], (texels[d], light)
                ).start()

    def column_start():
        for g, (pieces, plane, column, _) in enumerate(groups):
            others = pl.ds(1, n_texel - 1)
            copy(pieces.at[others], plane.at[others], plane_send.at[g], plane_recv.at[g], (texels[1], light)).wait()
            total = pieces[texel]
            for d in range(1, n_texel):
                total = total + plane[d]
            column[own_column] = total
            for d in range(1, n_light):
                copy(
                    column.at[own_column], column.at[own_column], column_send.at[g], column_recv.at[g],
                    (texel, lights[d]),
                ).start()

    def rows_start(g, coming):
        _, _, column, rows = groups[g]
        some = column.at[pl.ds(0, coming)]
        copy(some, some, column_send.at[g], column_recv.at[g], (texel, lights[1])).wait_recv()
        total = column[0]
        for index in range(1, owners):
            total = total + column[index]
        rows[texel] = total
        for d in range(1, n_texel):
            copy(rows.at[texel], rows.at[texel], row_send.at[g], row_recv.at[g], (texels[d], light)).start()

    def column_sent():
        for g in range(2):
            sent = groups[g][1].at[pl.ds(0, n_light - 1)]
            copy(sent, sent, column_send.at[g], column_recv.at[g], (texel, lights[1])).wait_send()

    @pl.when(inner == 0)
    def _():
        done, held_back = 0, ends * 5 // 8
        for c in range(ends):
            rows = rows_at(0, c, CHUNK)
            sum_copy(0, c, inward).wait_recv()
            whole[rows, :] = partial_ref[rows, :] + landed[chunk_of(0, c)]
            if c == held_back:
                all_sent(sum_send, capacity // CHUNK - ends)
                for earlier in range(c):
                    back_copy(0, earlier, inward).start()
            if c >= held_back:
                back_copy(0, c, inward).start()
            if c + 1 in (ends // 2, ends * 5 // 6, ends):
                add_gram(0, done, c + 1 - done)
                done = c + 1
        plane_start()
        split_rows(0)
        column_start()
        for g in range(2):
            rows_start(g, owners - 1)

    @pl.when(inner == 1)
    def _():
        for kind, o, c in relay_order(shares):
            if kind == "plane":
                add_gram(1, 0, owned)
                plane_start()
            elif kind == "column":
                column_start()
            elif kind == "rows":
                rows_start(c, owners - 1 if owned else owners)
            elif kind == "final":
                if c == 0:
                    copy(near, near, sum_send, near_recv, (texel, inward)).wait_recv()
                sum_copy(1, c, inward).wait_recv()
                rows = rows_at(1, c, CHUNK)
                whole[rows, :] = partial_ref[rows, :] + near[c] + landed[chunk_of(1, c)]
                back_copy(1, c, inward).start()
                back_copy(1, c, outward).start()
            elif kind == "inward" or kind == "outward":
                going = sum_copy(o, c, inward if kind == "inward" else outward)
                going.wait_recv()
                rows = rows_at(o, c, CHUNK)
                partial_ref[rows, :] = partial_ref[rows, :] + landed[chunk_of(o, c)]
                going.start()
            else:
                going = back_copy(o, c, inward if kind == "back_inward" else outward)
                going.wait_recv()
                going.start()
        for o in range(n_light):
            split_rows(o)

    def row_whole(g):
        others = groups[g][3].at[pl.ds(1, n_texel - 1)]
        return copy(others, others, row_send.at[g], row_recv.at[g], (texels[1], light))

    valid = counts_ref[0]
    for index in range(1, n_texel):
        valid = valid + counts_ref[index]
    valid = valid.astype(jnp.float32)
    row_whole(0).wait_recv()
    height = rows_first.shape[1]
    for index in range(n_texel):
        work[index * height : (index + 1) * height, :size] = rows_first[index] / valid

    def finish_gram():
        row_whole(1).wait_recv()
        height = rows_rest.shape[1]
        rest = jnp.concatenate([rows_rest[index] for index in range(n_texel)], axis=0) / valid
        work[quarter : 2 * quarter, :size] = rest[:quarter, :]
        work[2 * quarter :, : 2 * quarter] = jnp.zeros((2 * quarter, 2 * quarter), jnp.float32)
        work[2 * quarter : 3 * quarter, 2 * quarter : size] = rest[quarter:, : 2 * quarter]
        work[3 * quarter :, 2 * quarter : size] = rest[quarter:, 2 * quarter :]

    def finish_rows():
        @pl.when(inner == 0)
        def _():
            for o in range(1, n_light):
                for c in range(shares[o]):
                    back_copy(o, c, inward).wait_recv()
                split_rows(o)

    factor_inverse(work, finish_gram, finish_rows)
    inverse = split(work[:, size:])
    half_ref[...] = product(inverse, (high[...], low[...])).astype(jnp.bfloat16)

    def basis_rows(step):
        rows = slice(step * middle, (step + 1) * middle)
        basis_ref[rows, :] = product((high[rows, :], low[rows, :]), inverse)

    scatter_sum(
        n_texel, half_ref, tile_ref, product_ref, coeffs_ref, valid, held, arrived, out_send, out_recv, basis_rows
    )
    for half in range(2):
        sent = held.at[half, pl.ds(0, n_texel - 1)]
        copy(sent, sent, out_send.at[half], out_recv.at[half, 0], (texels[1], light)).wait_send()

    @pl.when(inner == 0)
    def _():
        all_sent(back_send, ends)
        column_sent()

    @pl.when(inner == 1)
    def _():
        all_sent(sum_send, 2 * ends + owned)
        all_sent(back_send, 2 * ends + 3 * owned)
        if owned:
            column_sent()

    for g in range(2):
        row_whole(g).wait_send()


def halving_order(bits, last_first):
    rest = list(range(1, bits))
    return [0] + (rest[::-1] if last_first else rest)


def scatter_sum(n_texel, half_ref, tile_ref, partial_ref, out_ref, valid, held, landed, send_sem, recv_sem, meanwhile):
    texel, light = lax.axis_index("texel"), lax.axis_index("light")
    bits = n_texel.bit_length() - 1
    bit = [lax.rem(texel // (1 << b), 2) for b in range(bits)]
    partner = [texel + (1 - 2 * bit[b]) * (1 << b) for b in range(bits)]
    piece = partial_ref.shape[0] // n_texel
    width = partial_ref.shape[1] // 2

    def start_of(mask):
        block = 0
        for b in range(bits):
            flipped = 1 - bit[b] if mask >> b & 1 else bit[b]
            block = block + flipped * (1 << b)
        return pl.multiple_of(block * piece, piece)

    def multiply(half):
        columns = slice(half * width, (half + 1) * width)
        partial_ref[:, columns] = lax.dot_general(
            half_ref[...], tile_ref[:, columns], (((1,), (0,)), ((), ())), preferred_element_type=jnp.float32
        )

    orders = [halving_order(bits, False), halving_order(bits, True)]
    root = jnp.sqrt(jnp.full((piece, width), valid))
    flights = [{}, {}]
    used = [0, 0]
    for step in range(bits):
        for half, order in enumerate(orders):
            if step == 0:
                multiply(half)
            b = order[step]
            left = [m for m in range(n_texel) if all(not m >> done & 1 for done in order[:step])]
            later = order[step + 1 :]
            going = [m for m in left if m >> b & 1]
            going.sort(key=lambda m: [-(m >> c & 1) for c in later])
            columns = pl.ds(half * width, width)
            for m in going:
                kept = m - (1 << b)
                if step == 0:
                    source = partial_ref.at[pl.ds(start_of(m), piece), columns]
                else:
                    arrived = flights[half].pop((step - 1, m))
                    arrived.wait_recv()
                    below = (
                        partial_ref[pl.ds(start_of(m), piece), columns] if step == 1 else held[half, m]
                    )
                    held[half, m] = below + landed[half, step - 1, m]
                    source = held.at[half, m]
                copy = pltpu.make_async_remote_copy(
                    src_ref=source,
                    dst_ref=landed.at[half, step, kept],
                    send_sem=send_sem.at[half],
                    recv_sem=recv_sem.at[half, used[half]],
                    device_id=(partner[b], light),
                    device_id_type=MESH_ID,
                )
                copy.start()
                used[half] += 1
                flights[half][step, kept] = copy
        if step == 1:
            meanwhile(0)
            meanwhile(1)
        if step:
            for half, order in enumerate(orders):
                for key in [k for k in flights[half] if k[0] == step - 1]:
                    m = key[1]
                    flights[half].pop(key).wait_recv()
                    columns = pl.ds(half * width, width)
                    below = (
                        partial_ref[pl.ds(start_of(m), piece), columns] if step == 1 else held[half, m]
                    )
                    held[half, m] = below + landed[half, step - 1, m]
    for half in range(2):
        columns = pl.ds(half * width, width)
        flights[half].pop((bits - 1, 0)).wait_recv()
        below = partial_ref[pl.ds(start_of(0), piece), columns] if bits == 1 else held[half, 0]
        out_ref[:, half * width : (half + 1) * width] = (below + landed[half, bits - 1, 0]) / root


def write_out(basis_ref, coeffs_ref, basis_out, coeffs_out, sems):
    parts = sems.shape[0] - 1
    height = basis_ref.shape[0] // parts
    copies = [pltpu.make_async_copy(coeffs_ref, coeffs_out, sems.at[parts])]
    for index in range(parts):
        rows = pl.ds(index * height, height)
        copies.append(pltpu.make_async_copy(basis_ref.at[rows], basis_out.at[rows], sems.at[index]))
    for going in copies:
        going.start()
    for going in copies:
        going.wait()


def on_device(n_texel, n_light, tex_feat, light_feat, sketch, row_counts):
    capacity, size = tex_feat.shape[0], sketch.shape[1]
    lights = light_feat.shape[0]
    block, step = capacity // 4, next(w for w in (256, 128) if lights % w == 0)
    shares, _ = layout_of(capacity, n_light)
    owners, piece = sum(1 for share in shares if share), size // n_texel
    first, rest = size // 4 // n_texel, size // 2 // n_texel
    width, bits = lights // 2, n_texel.bit_length() - 1
    vmem = pl.BlockSpec(memory_space=pltpu.VMEM)
    anywhere = pl.BlockSpec(memory_space=pl.ANY)
    f32, half = jnp.float32, jnp.bfloat16
    sems = pltpu.SemaphoreType.DMA
    basis, coeffs = pl.pallas_call(
        functools.partial(whole_step, n_texel, n_light),
        out_shape=(pltpu.VMEM((capacity, size), f32), pltpu.VMEM((piece, lights), f32)),
        in_specs=[anywhere] * 4,
        out_specs=(vmem, vmem),
        scratch_shapes=[
            pltpu.VMEM(tex_feat.shape, half),
            pltpu.VMEM(light_feat.shape, half),
            pltpu.VMEM(sketch.shape, half),
            pltpu.SMEM(row_counts.shape, jnp.int32),
            pltpu.VMEM((capacity, lights), half),
            pltpu.VMEM((size, capacity), half),
            pltpu.VMEM((size, lights), f32),
            pltpu.VMEM((2, n_texel, piece, width), f32),
            pltpu.VMEM((2, bits, n_texel, piece, width), f32),
            pltpu.VMEM((block, step), f32),
            pltpu.VMEM((block, step), f32),
            pltpu.VMEM((capacity, size), f32),
            pltpu.VMEM((capacity // CHUNK, CHUNK, size), f32),
            pltpu.VMEM((max(shares[1], 1), CHUNK, size), f32),
            pltpu.VMEM((capacity, size), f32),
            pltpu.VMEM((size, 2 * size), f32),
            pltpu.VMEM((size, size), f32),
            pltpu.VMEM((capacity, size), half),
            pltpu.VMEM((capacity, size), half),
            pltpu.VMEM((n_texel, first, size), f32), pltpu.VMEM((n_texel, rest, size), f32),
            pltpu.VMEM((n_texel, first, size), f32), pltpu.VMEM((n_texel, rest, size), f32),
            pltpu.VMEM((owners, first, size), f32), pltpu.VMEM((owners, rest, size), f32),
            pltpu.VMEM((n_texel, first, size), f32), pltpu.VMEM((n_texel, rest, size), f32),
            sems, sems, sems((capacity // CHUNK,)), sems,
            sems((2,)), sems((2,)),
            sems((2,)), sems((2,)),
            sems((2,)), sems((2,)),
            sems((2,)), sems((2, n_texel - 1)),
            sems((4,)), sems((5,)),
        ],
        compiler_params=pltpu.CompilerParams(collective_id=1, has_side_effects=True),
    )(tex_feat, light_feat, sketch, row_counts)
    return pl.pallas_call(
        write_out,
        out_shape=(jax.ShapeDtypeStruct((capacity, size), f32), jax.ShapeDtypeStruct((piece, lights), f32)),
        in_specs=[vmem, vmem],
        out_specs=(pl.BlockSpec(memory_space=pl.ANY),) * 2,
        scratch_shapes=[sems((5,))],
    )(*(pltpu.with_memory_space_constraint(x, pltpu.VMEM) for x in (basis, coeffs)))


def solution(mesh):
    placed = (P("texel", None), P("light", None), P("light", None), P())
    return jax.shard_map(
        functools.partial(on_device, mesh.shape["texel"], mesh.shape["light"]),
        mesh=mesh,
        in_specs=placed,
        out_specs=(P("texel", None), P("texel", "light")),
        check_vma=False,
    )
```
